256 devices in a mesh: group: 2 (over z), grid: 64 (over y, x), var: 2 (over core).
Axes of the slice: x: 8, y: 8, z: 2, core: 2. Of those that a mesh axis runs over, the one named last changes fastest.
The devices are a block of a 8x8x16 slice.
Arguments:
- tokens: bfloat16 [96, 768, 3, 512], P('group', 'grid'), parts along dimension 0, may hold values from -6 to 6
- key_mask: int32 [96, 768], P('group', 'grid'), parts along dimension 0, may hold values 0 or 1
- w_qkv: bfloat16 [3, 512, 512], P(None, None, 'var'), may hold values from -16 to 16
- w_proj: bfloat16 [512, 512], P('var'), may hold values from -0.25 to 0.25
- w_up: bfloat16 [512, 2048], P(None, 'var'), may hold values from -0.25 to 0.25
- w_down: bfloat16 [2048, 512], P('var'), may hold values from -0.125 to 0.125
- level_query: bfloat16 [13, 512], replicated, may hold values from -1200 to 1200
- w_dec_q: bfloat16 [512, 512], P(None, 'var'), may hold values from -0.25 to 0.25
- w_dec_kv: bfloat16 [2, 512, 512], P(None, None, 'var'), may hold values from -0.25 to 0.25
- w_dec_o: bfloat16 [512, 512], P('var'), may hold values from -0.25 to 0.25
- decode_matrix: float32 [512, 64], replicated, may hold values from -0.25 to 0.25
Outputs:
- estimated_maps: float32 [4, 26, 192, 3072], P('var', 'group', 'grid'), parts along dimension 1
The draws below stay inside these ranges and needn't reach their ends.
There are 2 independent parts, one for each index of `group`. The reference program is written for one: setup_inputs(seed, part) draws one part's arguments, and reference() takes and returns one part's arrays. A program takes and returns all parts, laid end to end along the dimension named above; an argument that names none is the same for every part. Nothing has to cross between parts.
All inputs are finite; a program needn't handle non-finite values. No bound on the sum of `key_mask` on one device may be relied on, other than what follows from the above.
Results may differ from the reference program's by a relative error of at most 0.025.
Values may be sent and summed in bfloat16 or wider, within the bound.
A program may use at most 128 MiB of HBM per device.

```python
import jax
import jax.numpy as jnp
from jax import lax

EMBED_WIDTH = 512
HD = 64
FF = 2048
TARGET_QUANTITY = 4
ISOBAR_NUMBER = 13
LEV = 3
SQUARE_SPAN = 4
WIN_LAT = 6
WINDOW_EASTWARD = 12
LAT = 48
LON = 768


def draw_w_qkv(key, part):
    key = jax.random.fold_in(key, 11)
    base_key = jax.random.fold_in(key, 0)
    result = jnp.clip(jax.random.normal(base_key, (3, EMBED_WIDTH, EMBED_WIDTH), jnp.float32), -6.0, 6.0) * EMBED_WIDTH ** (-0.5)
    return result.astype(jnp.bfloat16)


def draw_level_query(key, part):
    key = jax.random.fold_in(key, 23)
    base_key = jax.random.fold_in(key, 0)
    result = jnp.clip(jax.random.normal(base_key, (ISOBAR_NUMBER, EMBED_WIDTH), jnp.float32), -6.0, 6.0)
    return result.astype(jnp.bfloat16)


def touch_ends(array, rng, smallest, top_value):
    shape = array.shape
    spot = [jax.random.randint(jax.random.fold_in(rng, axis), (), 0, shape[axis]) for axis in range(len(shape))]
    array = array.at[tuple(spot)].set(smallest)
    longest = shape.index(max(shape))
    spot[longest] = (spot[longest] + 1) % shape[longest]
    return array.at[tuple(spot)].set(top_value)


def shard_levels(key, shape, pieces, low, high):
    level, own = 1.0, jax.random.fold_in(key, 6)
    for dim, blocks in pieces:
        heights = jnp.exp(jax.random.uniform(jax.random.fold_in(own, dim), (blocks,), jnp.float32, low / len(pieces), high / len(pieces)))
        level = level * jnp.repeat(heights, shape[dim] // blocks).reshape([-1 if axis == dim else 1 for axis in range(len(shape))])
    return level


def normal_values(key, dims, scale, bound, cuts=(), dtype=jnp.bfloat16):
    level = shard_levels(key, dims, cuts, -0.22, 0.18) if cuts else 1.0
    entries = jax.random.normal(key, dims, jnp.float32) * scale * level
    return jnp.minimum(jnp.maximum(entries, -bound), bound).astype(dtype)


def setup_inputs(seed: int = 0, part: int = 0) -> dict:
    streams_of = jax.random.split(jax.random.key(seed), 12)
    part_splits = jax.random.split(jax.random.fold_in(streams_of[11], part), 12)
    return {
        "tokens": normal_values(part_splits[0], (LAT, LON, LEV, EMBED_WIDTH), 1.0, 6.0, ((1, 64),)),
        "key_mask": touch_ends((jax.random.randint(part_splits[1], (LAT, LON), 0, 4) < 3).astype(jnp.int32), jax.random.fold_in(part_splits[1], 1), 0, 1),
        "w_qkv": draw_w_qkv(jax.random.fold_in(streams_of[11], 71), part),
        "w_proj": normal_values(streams_of[3], (EMBED_WIDTH, EMBED_WIDTH), EMBED_WIDTH ** -0.5, 0.25, ((0, 2),)),
        "w_up": normal_values(streams_of[4], (EMBED_WIDTH, FF), EMBED_WIDTH ** -0.5, 0.25, ((1, 2),)),
        "w_down": normal_values(streams_of[5], (FF, EMBED_WIDTH), FF ** -0.5, 0.125, ((0, 2),)),
        "level_query": draw_level_query(jax.random.fold_in(streams_of[11], 71), part),
        "w_dec_q": normal_values(streams_of[7], (EMBED_WIDTH, EMBED_WIDTH), EMBED_WIDTH ** -0.5, 0.25, ((1, 2),)),
        "w_dec_kv": normal_values(streams_of[8], (2, EMBED_WIDTH, EMBED_WIDTH), EMBED_WIDTH ** -0.5, 0.25, ((2, 2),)),
        "w_dec_o": normal_values(streams_of[9], (EMBED_WIDTH, EMBED_WIDTH), EMBED_WIDTH ** -0.5, 0.25, ((0, 2),)),
        "decode_matrix": normal_values(streams_of[10], (EMBED_WIDTH, TARGET_QUANTITY * SQUARE_SPAN * SQUARE_SPAN), EMBED_WIDTH ** -0.5, 0.25, (), jnp.float32),
    }


EPSILON = 1e-05

def layer_norm(values):
    center = values - lax.optimization_barrier(jnp.mean(values, axis=-1, keepdims=True))
    spread = lax.optimization_barrier(jnp.mean(center * center, axis=-1, keepdims=True))
    return center * lax.rsqrt(spread + EPSILON)

def window_attention(tile_tokens, key_marks, row_start, total_rows, w_qkv, w_proj):
    north_south_circles, columns, levels, features = tile_tokens.shape
    local_width = w_qkv.shape[2]
    head_count = local_width // HD
    normed = layer_norm(tile_tokens.astype(jnp.float32)).astype(jnp.bfloat16).reshape(-1, features)
    win_count = north_south_circles // WIN_LAT
    tok_count = WIN_LAT * columns * levels

    def project(which):
        result = jnp.dot(normed, w_qkv[which], preferred_element_type=jnp.float32)
        return result.astype(jnp.bfloat16).reshape(win_count, tok_count, head_count, HD)
    queries = project(0)
    key_heads = project(1)
    value_heads = project(2)
    scores = jnp.einsum('wqhd,wkhd->whqk', queries.astype(jnp.float32), key_heads.astype(jnp.float32)) * HD ** (-0.5)
    row_index = lax.broadcasted_iota(jnp.int32, (north_south_circles, columns, levels), 0).reshape(win_count, tok_count)
    region = row_index + row_start >= total_rows - WIN_LAT // 2
    open_key = jnp.broadcast_to(key_marks[:, :, None], (north_south_circles, columns, levels)).reshape(win_count, tok_count) > 0
    diagonal = lax.broadcasted_iota(jnp.int32, (tok_count, tok_count), 0) == lax.broadcasted_iota(jnp.int32, (tok_count, tok_count), 1)
    allowed = (region[:, :, None] == region[:, None, :]) & (open_key[:, None, :] | diagonal[None])
    scores = jnp.where(allowed[:, None], scores, jnp.float32(-1e+30))
    peak_score = lax.optimization_barrier(jnp.max(scores, axis=-1, keepdims=True))
    exp_scores = jnp.exp(scores - peak_score)
    weights = (exp_scores / lax.optimization_barrier(jnp.sum(exp_scores, axis=-1, keepdims=True))).astype(jnp.bfloat16)
    context = jnp.einsum('whqk,wkhd->wqhd', weights.astype(jnp.float32), value_heads.astype(jnp.float32))
    context = context.astype(jnp.bfloat16).reshape(-1, local_width)
    return jnp.dot(context, w_proj, preferred_element_type=jnp.float32).reshape(north_south_circles, columns, levels, features)

def level_decoder(latent, level_query, w_dec_q, w_dec_kv, w_dec_o):
    north_south_circles, columns, levels, features = latent.shape
    local_width = w_dec_kv.shape[2]
    head_count = local_width // HD
    patches = north_south_circles * columns
    normed = layer_norm(latent.astype(jnp.float32)).astype(jnp.bfloat16).reshape(-1, features)
    dkeys = jnp.dot(normed, w_dec_kv[0], preferred_element_type=jnp.float32).astype(jnp.bfloat16)
    dvals = jnp.dot(normed, w_dec_kv[1], preferred_element_type=jnp.float32).astype(jnp.bfloat16)
    dkeys = dkeys.reshape(patches, levels, head_count, HD)
    dvals = dvals.reshape(patches, levels, head_count, HD)
    dquery = jnp.dot(level_query, w_dec_q, preferred_element_type=jnp.float32).reshape(-1, head_count, HD)
    scores = jnp.einsum('lhd,pjhd->plhj', dquery, dkeys.astype(jnp.float32)) * HD ** (-0.5)
    peak_score = lax.optimization_barrier(jnp.max(scores, axis=-1, keepdims=True))
    exp_scores = jnp.exp(scores - peak_score)
    dweights = (exp_scores / lax.optimization_barrier(jnp.sum(exp_scores, axis=-1, keepdims=True))).astype(jnp.bfloat16)
    dcontext = jnp.einsum('plhj,pjhd->plhd', dweights.astype(jnp.float32), dvals.astype(jnp.float32))
    dcontext = dcontext.astype(jnp.bfloat16).reshape(-1, local_width)
    return jnp.dot(dcontext, w_dec_o, preferred_element_type=jnp.float32)

def reference(tokens, key_mask, w_qkv, w_proj, w_up, w_down, level_query, w_dec_q, w_dec_kv, w_dec_o, decode_matrix):
    north_south_circles, east_west_bands_set, levels, features = tokens.shape
    half_lat = WIN_LAT // 2
    half_lon = WINDOW_EASTWARD // 2
    block_count = east_west_bands_set // WINDOW_EASTWARD
    rolled = jnp.roll(tokens, (-half_lat, -half_lon), (0, 1))
    rolled_mask = jnp.roll(key_mask, (-half_lat, -half_lon), (0, 1))
    rolled = jnp.moveaxis(rolled.reshape(north_south_circles, block_count, WINDOW_EASTWARD, levels, features), 1, 0)
    rolled_mask = jnp.moveaxis(rolled_mask.reshape(north_south_circles, block_count, WINDOW_EASTWARD), 1, 0)

    def attend(block_pair):
        return window_attention(block_pair[0], block_pair[1], 0, north_south_circles, w_qkv, w_proj)
    attended = lax.map(attend, (rolled, rolled_mask))
    attended = jnp.moveaxis(attended, 0, 1).reshape(north_south_circles, east_west_bands_set, levels, features)
    attended = jnp.roll(attended, (half_lat, half_lon), (0, 1))
    x_one = tokens.astype(jnp.float32) + attended
    x_blocks = jnp.moveaxis(x_one.reshape(north_south_circles, block_count, WINDOW_EASTWARD, levels, features), 1, 0)

    def finish(x_block):
        normed = layer_norm(x_block).astype(jnp.bfloat16)
        hidden = jax.nn.gelu(jnp.dot(normed, w_up, preferred_element_type=jnp.float32), approximate=False).astype(jnp.bfloat16)
        latent = (x_block + jnp.dot(hidden, w_down, preferred_element_type=jnp.float32)).astype(jnp.bfloat16)
        dec_hidden = level_decoder(latent, level_query, w_dec_q, w_dec_kv, w_dec_o)
        cell_measures = jnp.dot(dec_hidden, decode_matrix, precision=lax.Precision.HIGHEST, preferred_element_type=jnp.float32)
        return cell_measures.reshape(north_south_circles, WINDOW_EASTWARD, ISOBAR_NUMBER, TARGET_QUANTITY, SQUARE_SPAN, SQUARE_SPAN)
    cell_measures = lax.map(finish, x_blocks)
    estimated_maps = jnp.transpose(cell_measures, (4, 3, 1, 5, 0, 2, 6))
    return estimated_maps.reshape(TARGET_QUANTITY, ISOBAR_NUMBER, north_south_circles * SQUARE_SPAN, east_west_bands_set * SQUARE_SPAN)
```

```python
import functools

import jax
import jax.numpy as jnp
import numpy as np
from jax import lax
from jax.experimental import pallas as pl
from jax.experimental.pallas import tpu as pltpu
from jax.sharding import PartitionSpec as P

HD = 64
WIN = 6
LEV = 3
PIX = 4
NLEV = 13
HALF = 112
TOK = 2 * HALF
EPSILON = 1e-05
LOG2E = 1.4426950408889634
NEG = -1e30
BF = jnp.bfloat16
F32 = jnp.float32


def sizes(grid):
    dests = grid // 8
    band = WIN * PIX // dests
    rows = -(-(band * 12) // 8) * 8
    return dests, band, rows


def token_fields():
    t = np.arange(TOK)
    half, q = t // HALF, t % HALF
    valid = q < 108
    cj, r = q // 6, q % 6
    return half, cj // 3, cj % 3, r, valid


def main_tables(grid):
    dests, band, rows = sizes(grid)
    pick = np.zeros((192, 256), np.float32)
    pick2 = np.zeros((64, 64), np.float32)
    for w in range(4):
        for r in range(6):
            for cj in range(8):
                pick[w * 48 + cj * 6 + r, cj * 32 + 3 + 6 * w + r] = 1
            for cj in range(2):
                pick2[w * 16 + cj * 6 + r, cj * 32 + 3 + 6 * w + r] = 1
    half, c6, j, r, valid = token_fields()
    level_rows = np.zeros((384, TOK), np.float32)
    t = np.arange(TOK)[valid]
    patch = half * 36 + c6 * 6 + r
    level_rows[j[valid] * 128 + patch[valid], t] = 1
    out_rows = np.zeros((4, dests * rows, 128), np.float32)
    for d in range(dests):
        for slot in range(band):
            rr, a = divmod(band * d + slot, 4)
            for c in range(12):
                out_rows[a, d * rows + slot * 12 + c, (c // 6) * 36 + (c % 6) * 6 + rr] = 1
    mask_rows = np.zeros((8, 48, TOK), np.float32)
    for window in range(8):
        mask_rows[window, ((6 * window + 3 + r) % 48)[valid], t] = 1
    mask_cols = np.zeros((32, TOK), np.float32)
    mask_cols[np.where(half == 0, 6 + c6, 16 + c6)[valid], t] = 1
    seam = np.where((r >= 3)[:, None] == (r >= 3)[None, :], 0, NEG).astype(np.float32)
    order = np.zeros((64, 64), np.float32)
    for a in range(4):
        for vh in range(2):
            for b in range(4):
                for v in range(2):
                    order[((a * 2 + vh) * 4 + b) * 2 + v, ((vh * 2 + v) * 4 + a) * 4 + b] = 1
    return (
        jnp.asarray(pick, BF),
        jnp.asarray(pick2, BF),
        jnp.asarray(level_rows, BF),
        jnp.asarray(out_rows, BF),
        jnp.asarray(mask_rows, BF),
        jnp.asarray(mask_cols, F32),
        jnp.asarray(seam, F32),
        jnp.asarray(order, BF),
    )


def dot(a, b):
    return lax.dot_general(a, b, (((1,), (0,)), ((), ())), preferred_element_type=F32)


def dot_t(a, b):
    return lax.dot_general(a, b, (((1,), (1,)), ((), ())), preferred_element_type=F32)


def norm(values):
    center = values - jnp.mean(values, axis=-1, keepdims=True)
    spread = jnp.mean(center * center, axis=-1, keepdims=True)
    return (center * lax.rsqrt(spread + EPSILON)).astype(BF)


def split3(values):
    hi = values.astype(BF)
    rest = values - hi.astype(F32)
    mid = rest.astype(BF)
    return hi, mid, (rest - mid.astype(F32)).astype(BF)


def main_kernel(
    grid,
    tokens, mask, w_qkv, w_proj, w_up, w_down, query, w_dec_q, w_dec_kv, w_dec_o, decode_t,
    c_pick, c_pick2, c_level, c_out, c_mrow, c_mcol, c_seam, c_order,
    recv,
    tok, own, hsend, hrecv, b_qkv, b_proj, b_up, b_down, b_kt, b_gt, b_dq, qbd,
    v_query, v_dq, v_dkv, v_do, v_dec, pick, pick2, level, outm, mrow, mcol, seam, order,
    mask_own, mask_right, marks, hidden, diff, dwt, zpix, msg,
    lsem, wsend, wrecv, hssem, hrsem, osend, orecv,
):
    dests, band, rows = sizes(grid)
    me = lax.axis_index("grid")
    v = lax.axis_index("var")
    partner = {"var": 1 - v}
    west = {"grid": lax.rem(me + grid - 1, grid)}

    barrier = pltpu.get_barrier_semaphore()
    flat = me * 2 + v

    def greet(k, _):
        other = lax.rem(flat + k, 2 * grid)
        pl.semaphore_signal(
            barrier, inc=1, device_id={"grid": other // 2, "var": lax.rem(other, 2)}, device_id_type=pl.DeviceIdType.MESH
        )
        return 0

    lax.fori_loop(1, 2 * grid, greet, 0)

    row0 = pl.multiple_of(24 * v, 8)
    row1 = pl.multiple_of(lax.rem(24 * v + 24, 48), 8)
    loads = [
        (tokens.at[:, pl.ds(row0, 24), :], tok.at[:, pl.ds(0, 24), :]),
        (tokens.at[:, pl.ds(row1, 8), :], tok.at[:, pl.ds(24, 8), :]),
        (c_pick, pick),
        (c_pick2, pick2),
        (w_dec_o, v_do),
        (decode_t, v_dec),
        (c_order, order),
        (w_dec_kv, v_dkv),
        (query, v_query),
        (w_dec_q, v_dq),
        (mask, mask_own),
        (w_qkv, b_qkv.at[v]),
        (c_mrow, mrow),
        (c_mcol, mcol),
        (c_seam, seam),
        (w_proj, b_proj.at[v]),
        (w_up, b_up.at[v]),
        (w_down, b_down.at[v]),
        (c_level, level),
        (c_out, outm),
    ]
    local = [pltpu.make_async_copy(src, dst, lsem.at[i]) for i, (src, dst) in enumerate(loads)]
    for copy in local:
        copy.start()

    for i in range(4):
        local[i].wait()
    for part, target in ((0, hsend), (18, own)):
        for block in range(2):
            src = tok[part + 8 * block : part + 8 * block + 8].reshape(256, 512)
            packed = dot(pick[...], src).astype(BF)
            for w in range(4):
                target[w, 48 * block : 48 * block + 48, :] = packed[48 * w : 48 * w + 48]
        src = tok[part + 16 : part + 18].reshape(64, 512)
        packed = dot(pick2[...], src).astype(BF)
        for w in range(4):
            target[w, 96:112, :] = packed[16 * w : 16 * w + 16]

    for i in range(4, 10):
        local[i].wait()
    dec = v_dec[...]
    hi, mid, low = split3(dec)
    do = v_do[...]
    unembed = (dot_t(hi, do) + dot_t(mid, do) + dot_t(low, do)).astype(BF)
    unembed = dot(order[...], unembed).astype(BF)
    lane = lax.broadcasted_iota(jnp.int32, (64, 256), 1)
    for h in range(4):
        block = jnp.where((lane >= 64 * h) & (lane < 64 * h + 64), unembed.astype(F32), 0).astype(BF)
        b_gt[v, 64 * h : 64 * h + 64, :] = dot_t(block, v_dkv[1]).astype(BF)
    eye = jnp.where(
        lax.broadcasted_iota(jnp.int32, (256, 256), 0) == lax.broadcasted_iota(jnp.int32, (256, 256), 1), 1.0, 0.0
    ).astype(BF)
    b_kt[v] = dot_t(eye, v_dkv[0]).astype(BF)
    b_dq[v, 0:13, :] = dot(v_query[...], v_dq[...])
    b_dq[v, 13:16, :] = jnp.zeros((3, 256), F32)

    pl.semaphore_wait(barrier, 2 * grid - 1)

    def remote(src, dst, send, recv_sem, where):
        return pltpu.make_async_remote_copy(
            src_ref=src, dst_ref=dst, send_sem=send, recv_sem=recv_sem, device_id=where, device_id_type=pl.DeviceIdType.MESH
        )

    def halo(w):
        return remote(hsend.at[w], hrecv.at[w], hssem.at[w], hrsem.at[w], west)

    mask_copy = remote(mask, mask_right, hssem.at[4], hrsem.at[4], west)
    mask_copy.start()
    for step in range(4):
        halo(lax.rem(me + 3 + step, 4)).start()
    weights = [
        (w_qkv, b_qkv.at[v]),
        (w_proj, b_proj.at[v]),
        (w_up, b_up.at[v]),
        (w_down, b_down.at[v]),
        (b_kt.at[v], b_kt.at[v]),
        (b_gt.at[v], b_gt.at[v]),
        (b_dq.at[v], b_dq.at[v]),
    ]
    shared = [remote(src, dst, wsend.at[i], wrecv.at[i], partner) for i, (src, dst) in enumerate(weights)]
    for copy in shared:
        copy.start()
    zpix[...] = jnp.zeros_like(zpix)
    marks[...] = jnp.zeros_like(marks)

    for i in range(10, len(local)):
        local[i].wait()
    mask_copy.wait()
    marks[0:12, :] = mask_own[...].astype(F32)
    marks[16:28, :] = mask_right[...].astype(F32)
    for copy in shared:
        copy.wait()
    lane2 = lax.broadcasted_iota(jnp.int32, (16, 256), 1)
    for g in range(2):
        dq = b_dq[g] * (HD ** -0.5)
        for h in range(4):
            part = jnp.where((lane2 >= 64 * h) & (lane2 < 64 * h + 64), dq, 0.0)
            hi = part.astype(BF)
            qbd[g, 16 * h : 16 * h + 16, :] = hi
            qbd[g, 64 + 16 * h : 80 + 16 * h, :] = (part - hi.astype(F32)).astype(BF)

    pair_lane = lax.broadcasted_iota(jnp.int32, (TOK, 128), 1)
    ones = jnp.ones((TOK, 128), BF)

    def window(step, _):
        w = lax.rem(me + step, 4)
        halo(w).wait_recv()
        x = jnp.concatenate([own[w], hrecv[w]], axis=0).astype(F32)
        n1 = norm(x)
        kept = jnp.sum(dot(marks[...].astype(BF), mrow[4 * v + w]) * mcol[...], axis=0, keepdims=True)
        last = jnp.where(4 * v + w == 7, 1.0, 0.0)
        bias = seam[...] * last + jnp.where(kept > 0.5, 0.0, NEG)
        diagonal = lax.broadcasted_iota(jnp.int32, (TOK, TOK), 0) == lax.broadcasted_iota(jnp.int32, (TOK, TOK), 1)
        bias = jnp.where(diagonal, 0.0, bias)
        attended = jnp.zeros((TOK, 512), F32)
        for g in range(2):
            q = (dot(n1, b_qkv[g, 0]).astype(BF)) * BF(HD ** -0.5)
            k = dot(n1, b_qkv[g, 1]).astype(BF)
            val = dot(n1, b_qkv[g, 2]).astype(BF)
            contexts = []
            for pair in range(2):
                cut = slice(128 * pair, 128 * pair + 128)
                context = None
                for side in range(2):
                    inside = (pair_lane >= 64 * side) & (pair_lane < 64 * side + 64)
                    qs = jnp.where(inside, q[:, cut], BF(0))
                    vs = jnp.where(inside, val[:, cut], BF(0))
                    scores = dot_t(qs, k[:, cut]) + bias
                    top = jnp.max(scores, axis=-1, keepdims=True)
                    probs = jnp.exp2((scores - top) * LOG2E).astype(BF)
                    both = dot(probs, jnp.concatenate([vs, ones], axis=1))
                    part = both[:, :128] * (1.0 / both[:, 128:])
                    context = part if context is None else context + part
                contexts.append(context.astype(BF))
            attended = attended + dot(jnp.concatenate(contexts, axis=1), b_proj[g])
        x1 = x + attended
        n2 = norm(x1)
        for g in range(2):
            for c in range(2):
                h = dot(n2, b_up[g, :, 512 * c : 512 * c + 512])
                h = 0.5 * h * (1.0 + lax.erf(h * (2.0 ** -0.5)))
                hidden[:, 1024 * g + 512 * c : 1024 * g + 512 * c + 512] = h.astype(BF)
        grown = x1 + dot(hidden[:, :1024], b_down[0]) + dot(hidden[:, 1024:], b_down[1])
        n3 = norm(grown.astype(BF).astype(F32))
        by_level = dot(level[...], n3).astype(BF)
        base = jnp.zeros((64, 128), F32)
        for g in range(2):
            kt = dot_t(b_kt[g], by_level).astype(BF)
            both = dot(qbd[g], kt)
            scores = both[:64] + both[64:]
            s0, s1, s2 = scores[:, :128], scores[:, 128:256], scores[:, 256:]
            top = jnp.maximum(jnp.maximum(s0, s1), s2)
            e0, e1, e2 = (jnp.exp2((s - top) * LOG2E) for s in (s0, s1, s2))
            scale = 1.0 / (e0 + e1 + e2)
            dwt[g, 0] = e0 * scale
            dwt[g, 1] = e1 * scale
            vals = dot_t(b_gt[g], by_level)
            last_level = vals[:, 256:]
            d0, d1 = vals[:, :128] - last_level, vals[:, 128:256] - last_level
            for h in range(4):
                diff[g, h, 0] = d0[64 * h : 64 * h + 64]
                diff[g, h, 1] = d1[64 * h : 64 * h + 64]
                base = base + last_level[64 * h : 64 * h + 64]
        for l in range(NLEV):
            total = base
            for g in range(2):
                for h in range(4):
                    for j in range(2):
                        total = total + dwt[g, j, 16 * h + l : 16 * h + l + 1, :] * diff[g, h, j]
            zpix[pl.ds(l, 64, stride=16), :] = total
        packed = jnp.zeros((dests * rows, 256), F32)
        for a in range(4):
            packed = packed + dot_t(outm[a], zpix[256 * a : 256 * a + 256, :].astype(BF))
        for d in range(dests):
            for side in range(2):
                msg[w, side, d] = packed[rows * d : rows * d + rows, 128 * side : 128 * side + 128].astype(BF)
        for d in range(dests):
            to = lax.rem((4 * v + w) * dests + dests // 2 + d, grid)
            for side in range(2):
                mine = (to == me) & (v == side)

                @pl.when(mine)
                def _():
                    pltpu.make_async_copy(msg.at[w, side, d], recv.at[me], orecv).start()

                @pl.when(jnp.logical_not(mine))
                def _():
                    remote(msg.at[w, side, d], recv.at[me], osend, orecv, {"grid": to, "var": side}).start()

        return 0

    lax.fori_loop(0, 4, window, 0)
    for w in range(4):
        halo(w).wait_send()
    my_window = lax.rem(me + grid - dests // 2, grid) // dests
    stays = my_window // 4 == v
    pltpu.make_async_copy(recv, recv, orecv).wait()

    @pl.when(stays)
    def _():
        part = recv.at[pl.ds(0, grid - 1)]
        pltpu.make_async_copy(part, part, osend).wait()

    @pl.when(jnp.logical_not(stays))
    def _():
        pltpu.make_async_copy(recv, recv, osend).wait()


def final_tables(grid):
    _, band, _ = sizes(grid)
    pad = -(-26 * band // 16) * 16
    rows = np.zeros((band, 4 * pad, 128), np.float32)
    for slot in range(band):
        for b in range(4):
            for l in range(NLEV):
                for v in range(2):
                    rows[slot, b * pad + (l * band + slot) * 2 + v, (b * 2 + v) * 16 + l] = 1
    tile = np.gcd(12 * grid, 128)
    spread = np.zeros((4, tile, 4 * tile), np.float32)
    for b in range(4):
        spread[b, np.arange(tile), 4 * np.arange(tile) + b] = 1
    return jnp.asarray(rows, BF), jnp.asarray(spread.reshape(2, 2 * tile, 4 * tile), BF)


def final_kernel(grid, recv, sel, spread, out, stage):
    _, band, _ = sizes(grid)
    cells = 12 * grid
    pad = sel.shape[1] // 4
    for s in range(grid):
        block = recv[s].astype(F32)
        start = 12 * s + 6
        for slot in range(band):
            piece = block[12 * slot : 12 * slot + 12]
            if start + 12 <= cells:
                stage[slot, start : start + 12, :] = piece
            else:
                stage[slot, start : start + 6, :] = piece[:6]
                stage[slot, 0:6, :] = piece[6:]
    flipped = jnp.zeros((4 * pad, cells), F32)
    for slot in range(band):
        flipped = flipped + dot_t(sel[slot], stage[slot].astype(BF))
    flipped = flipped.astype(BF)
    tile = spread.shape[2] // 4
    tiles = cells // tile

    def stacked(b):
        return jnp.concatenate(
            [flipped[b * pad : b * pad + pad, tile * m : tile * m + tile] for m in range(tiles)], axis=0
        )

    lines = dot(jnp.concatenate([stacked(0), stacked(1)], axis=1), spread[0]) + dot(
        jnp.concatenate([stacked(2), stacked(3)], axis=1), spread[1]
    )
    for m in range(tiles):
        for k in range(NLEV * band):
            out[k, :, 4 * tile * m : 4 * tile * (m + 1)] = lines[m * pad + 2 * k : m * pad + 2 * k + 2]


def pixels_of(grid, tokens, key_mask, w_qkv, w_proj, w_up, w_down, level_query, w_dec_q, w_dec_kv, w_dec_o, decode_matrix):
    dests, band, rows = sizes(grid)
    by_column = jnp.transpose(tokens, (1, 2, 0, 3)).reshape(36, 48, 512)
    tables = main_tables(grid)
    operands = (
        by_column, key_mask.T, w_qkv, w_proj, w_up, w_down, level_query, w_dec_q, w_dec_kv, w_dec_o, decode_matrix.T,
    ) + tables
    vm = pltpu.VMEM
    return pl.pallas_call(
        functools.partial(main_kernel, grid),
        out_shape=jax.ShapeDtypeStruct((grid, rows, 128), BF),
        in_specs=[pl.BlockSpec(memory_space=pl.ANY)] * len(operands),
        out_specs=pl.BlockSpec(memory_space=pl.ANY),
        scratch_shapes=[
            vm((36, 32, 512), BF),
            vm((4, HALF, 512), BF),
            vm((4, HALF, 512), BF),
            vm((4, HALF, 512), BF),
            vm((2, 3, 512, 256), BF),
            vm((2, 256, 512), BF),
            vm((2, 512, 1024), BF),
            vm((2, 1024, 512), BF),
            vm((2, 256, 512), BF),
            vm((2, 256, 512), BF),
            vm((2, 16, 256), F32),
            vm((2, 128, 256), BF),
            vm((13, 512), BF),
            vm((512, 256), BF),
            vm((2, 512, 256), BF),
            vm((256, 512), BF),
            vm((64, 512), F32),
            *[vm(table.shape, table.dtype) for table in tables],
            vm((12, 48), jnp.int32),
            vm((12, 48), jnp.int32),
            vm((32, 48), F32),
            vm((TOK, 2048), BF),
            vm((2, 4, 2, 64, 128), F32),
            vm((2, 2, 64, 128), F32),
            vm((1024, 128), F32),
            vm((4, 2, dests, rows, 128), BF),
            pltpu.SemaphoreType.DMA((20,)),
            pltpu.SemaphoreType.DMA((7,)),
            pltpu.SemaphoreType.DMA((7,)),
            pltpu.SemaphoreType.DMA((5,)),
            pltpu.SemaphoreType.DMA((5,)),
            pltpu.SemaphoreType.DMA,
            pltpu.SemaphoreType.DMA,
        ],
        compiler_params=pltpu.CompilerParams(
            collective_id=0, has_side_effects=True, vmem_limit_bytes=60 * 2**20
        ),
    )(*operands)


def assemble(grid, received):
    _, band, _ = sizes(grid)
    tables = final_tables(grid)
    lines = pl.pallas_call(
        functools.partial(final_kernel, grid),
        out_shape=jax.ShapeDtypeStruct((NLEV * band, 2, 48 * grid), F32),
        scratch_shapes=[pltpu.VMEM((band, 12 * grid, 128), F32)],
        compiler_params=pltpu.CompilerParams(vmem_limit_bytes=60 * 2**20),
    )(received, *tables)
    return jnp.transpose(lines.reshape(NLEV, band, 2, 48 * grid), (2, 0, 1, 3))


def local(*args):
    grid = lax.axis_size("grid")
    return assemble(grid, pixels_of(grid, *args))


def solution(mesh):
    placed = (
        P("group", "grid", None, None),
        P("group", "grid"),
        P(None, None, "var"),
        P("var", None),
        P(None, "var"),
        P("var", None),
        P(),
        P(None, "var"),
        P(None, None, "var"),
        P("var", None),
        P(),
    )
    return jax.shard_map(
        local, mesh=mesh, in_specs=placed, out_specs=P("var", "group", "grid", None), check_vma=False
    )
```

```python
import functools

import jax
import jax.numpy as jnp
import numpy as np
from jax import lax
from jax.experimental import pallas as pl
from jax.experimental.pallas import tpu as pltpu
from jax.sharding import PartitionSpec as P

HD = 64
WIN = 6
LEV = 3
PIX = 4
NLEV = 13
HALF = 112
TOK = 2 * HALF
EPSILON = 1e-05
LOG2E = 1.4426950408889634
NEG = -1e30
BF = jnp.bfloat16
F32 = jnp.float32


SLOTS = 4


def window_of(v, slot):
    return (7 * v + 2 * slot) % 8


def sizes(grid):
    dests = grid // 8
    band = WIN * PIX // dests
    rows = -(-(band * 12) // 8) * 8
    return dests, band, rows


def reach(grid):
    stride = int(round(grid**0.5)) if grid > 8 else 2
    radius = 0
    for k in range(grid):
        ways = [abs(b) + min((k - stride * b) % grid, (stride * b - k) % grid) for b in range(-stride, stride + 1)]
        radius = max(radius, min(ways))
    rounds = max(0, (radius - 1).bit_length())
    assert rounds <= 3
    return stride, rounds


def token_fields():
    t = np.arange(TOK)
    half, q = t // HALF, t % HALF
    valid = q < 108
    cj, r = q // 6, q % 6
    return half, cj // 3, cj % 3, r, valid


def main_tables(grid):
    dests, band, rows = sizes(grid)
    pick = np.zeros((2, SLOTS * 48, 8 * 48), np.float32)
    pick2 = np.zeros((2, SLOTS * 16, 2 * 48), np.float32)
    for v in range(2):
        for step in range(SLOTS):
            for r in range(6):
                row = (6 * int(window_of(v, step)) + 3 + r) % 48
                for cj in range(8):
                    pick[v, step * 48 + cj * 6 + r, cj * 48 + row] = 1
                for cj in range(2):
                    pick2[v, step * 16 + cj * 6 + r, cj * 48 + row] = 1
    half, c6, j, r, valid = token_fields()
    level_rows = np.zeros((384, TOK), np.float32)
    t = np.arange(TOK)[valid]
    patch = half * 36 + c6 * 6 + r
    level_rows[j[valid] * 128 + patch[valid], t] = 1
    out_rows = np.zeros((4, dests * rows, 128), np.float32)
    for d in range(dests):
        for slot in range(band):
            rr, a = divmod(band * d + slot, 4)
            for c in range(12):
                out_rows[a, d * rows + slot * 12 + c, (c // 6) * 36 + (c % 6) * 6 + rr] = 1
    mask_rows = np.zeros((8, 48, TOK), np.float32)
    for window in range(8):
        mask_rows[window, ((6 * window + 3 + r) % 48)[valid], t] = 1
    mask_cols = np.zeros((32, TOK), np.float32)
    mask_cols[np.where(half == 0, 6 + c6, 16 + c6)[valid], t] = 1
    seam = np.where((r >= 3)[:, None] == (r >= 3)[None, :], 0, NEG).astype(np.float32)
    order = np.zeros((64, 64), np.float32)
    for a in range(4):
        for vh in range(2):
            for b in range(4):
                for v in range(2):
                    order[((a * 2 + vh) * 4 + b) * 2 + v, ((vh * 2 + v) * 4 + a) * 4 + b] = 1
    return (
        jnp.asarray(pick, BF),
        jnp.asarray(pick2, BF),
        jnp.asarray(level_rows, BF),
        jnp.asarray(out_rows, BF),
        jnp.asarray(mask_rows, BF),
        jnp.asarray(mask_cols, F32),
        jnp.asarray(seam, F32),
        jnp.asarray(order, BF),
    )


def dot(a, b):
    return lax.dot_general(a, b, (((1,), (0,)), ((), ())), preferred_element_type=F32)


def dot_t(a, b):
    return lax.dot_general(a, b, (((1,), (1,)), ((), ())), preferred_element_type=F32)


def norm(values):
    center = values - jnp.mean(values, axis=-1, keepdims=True)
    spread = jnp.mean(center * center, axis=-1, keepdims=True)
    return (center * lax.rsqrt(spread + EPSILON)).astype(BF)


def split3(values):
    hi = values.astype(BF)
    rest = values - hi.astype(F32)
    mid = rest.astype(BF)
    return hi, mid, (rest - mid.astype(F32)).astype(BF)


def main_kernel(
    grid,
    tokens, mask, w_qkv, w_proj, w_up, w_down, query, w_dec_q, w_dec_kv, w_dec_o, decode_t,
    c_pick, c_pick2, c_level, c_out, c_mrow, c_mcol, c_seam, c_order,
    recv,
    tok, own, hsend, hrecv, xone, b_qkv, b_proj, b_up, b_down, b_kg, b_dq, qbd,
    v_query, v_dq, v_dkv, v_do, v_dec, pick, pick2, level, outm, mrow, mcol, seam, order,
    mask_own, mask_right, marks, hidden, diff, dwt, zpix, msg,
    lsem, wsend, wrecv, hssem, hrsem, osend, orecv, heard,
):
    dests, band, rows = sizes(grid)
    me = lax.axis_index("grid")
    v = lax.axis_index("var")
    partner = {"var": 1 - v}
    west = {"grid": lax.rem(me + grid - 1, grid)}

    barrier = pltpu.get_barrier_semaphore()

    def signal(sem, where):
        pl.semaphore_signal(sem, inc=1, device_id=where, device_id_type=pl.DeviceIdType.MESH)

    stride, rounds = reach(grid)
    sides = (1, grid - 1, stride, grid - stride)
    signal(barrier, partner)
    for by in sides:
        signal(barrier, {"grid": lax.rem(me + by, grid)})

    def tell(k):
        if k < rounds:
            for by in sides:
                signal(heard.at[k], {"grid": lax.rem(me + by * 2**k, grid)})
        elif k == rounds:
            signal(heard.at[k], partner)

    def hear(k):
        if k <= rounds:
            pl.semaphore_wait(heard.at[k], 4 if k < rounds else 1)

    loads = [
        (tokens.at[pl.ds(0, 18)], tok.at[pl.ds(0, 18)]),
        (c_pick.at[v], pick),
        (c_pick2.at[v], pick2),
        (tokens.at[pl.ds(18, 18)], tok.at[pl.ds(18, 18)]),
        (w_dec_o, v_do),
        (decode_t, v_dec),
        (c_order, order),
        (w_dec_kv, v_dkv),
        (query, v_query),
        (w_dec_q, v_dq),
        (mask, mask_own),
        (w_qkv, b_qkv.at[v]),
        (c_mrow, mrow),
        (c_mcol, mcol),
        (c_seam, seam),
        (w_proj, b_proj.at[v]),
        (w_up, b_up.at[v]),
        (w_down, b_down.at[v]),
        (c_level, level),
        (c_out, outm),
    ]
    local = [pltpu.make_async_copy(src, dst, lsem.at[i]) for i, (src, dst) in enumerate(loads)]
    for copy in local:
        copy.start()

    def remote(src, dst, send, recv_sem, where):
        return pltpu.make_async_remote_copy(
            src_ref=src, dst_ref=dst, send_sem=send, recv_sem=recv_sem, device_id=where, device_id_type=pl.DeviceIdType.MESH
        )

    def halo(w):
        return remote(hsend.at[w], hrecv.at[w], hssem.at[w], hrsem.at[w], west)

    weights = [
        (w_qkv, b_qkv.at[v]),
        (w_proj, b_proj.at[v]),
        (w_up, b_up.at[v]),
        (w_down, b_down.at[v]),
        (b_kg.at[v], b_kg.at[v]),
        (b_kg.at[2 + v], b_kg.at[2 + v]),
        (b_dq.at[v], b_dq.at[v]),
    ]
    shared = [remote(src, dst, wsend.at[i], wrecv.at[i], partner) for i, (src, dst) in enumerate(weights)]
    mask_copy = remote(mask, mask_right, hssem.at[SLOTS], hrsem.at[SLOTS], west)

    def pack(part, target):
        for block in range(2):
            src = tok[part + 8 * block : part + 8 * block + 8].reshape(384, 512)
            packed = dot(pick[...], src).astype(BF)
            for w in range(SLOTS):
                target[w, 48 * block : 48 * block + 48, :] = packed[48 * w : 48 * w + 48]
        src = tok[part + 16 : part + 18].reshape(96, 512)
        packed = dot(pick2[...], src).astype(BF)
        for w in range(SLOTS):
            target[w, 96:112, :] = packed[16 * w : 16 * w + 16]

    pl.semaphore_wait(barrier, 5)
    for copy in shared[:4]:
        copy.start()
    mask_copy.start()
    tell(0)

    for i in range(3):
        local[i].wait()
    pack(0, hsend)
    for step in range(SLOTS):
        halo(lax.rem(me + grid - 1 + step, SLOTS)).start()
    local[3].wait()
    pack(18, own)

    for i in range(4, 10):
        local[i].wait()
    dec = v_dec[...]
    hi, mid, low = split3(dec)
    do = v_do[...]
    unembed = (dot_t(hi, do) + dot_t(mid, do) + dot_t(low, do)).astype(BF)
    unembed = dot(order[...], unembed).astype(BF)
    lane = lax.broadcasted_iota(jnp.int32, (64, 256), 1)
    for h in range(4):
        block = jnp.where((lane >= 64 * h) & (lane < 64 * h + 64), unembed.astype(F32), 0).astype(BF)
        b_kg[2 + v, 64 * h : 64 * h + 64, :] = dot_t(block, v_dkv[1]).astype(BF)
    eye = jnp.where(
        lax.broadcasted_iota(jnp.int32, (256, 256), 0) == lax.broadcasted_iota(jnp.int32, (256, 256), 1), 1.0, 0.0
    ).astype(BF)
    b_kg[v] = dot_t(eye, v_dkv[0]).astype(BF)
    b_dq[v, 0:13, :] = dot(v_query[...], v_dq[...])
    b_dq[v, 13:16, :] = jnp.zeros((3, 256), F32)

    for copy in shared[4:]:
        copy.start()
    hear(0)
    tell(1)
    zpix[...] = jnp.zeros_like(zpix)
    marks[...] = jnp.zeros_like(marks)

    for i in range(10, len(local)):
        local[i].wait()
    mask_copy.wait()
    marks[0:12, :] = mask_own[...].astype(F32)
    marks[16:28, :] = mask_right[...].astype(F32)
    pair_lane = lax.broadcasted_iota(jnp.int32, (TOK, 128), 1)
    ones = jnp.ones((TOK, 128), BF)

    def attend(w):
        which = window_of(v, w)
        x = jnp.concatenate([own[w], hrecv[w]], axis=0).astype(F32)
        n1 = norm(x)
        kept = jnp.sum(dot(marks[...].astype(BF), mrow[which]) * mcol[...], axis=0, keepdims=True)
        last = jnp.where(which == 7, 1.0, 0.0)
        bias = seam[...] * last + jnp.where(kept > 0.5, 0.0, NEG)
        diagonal = lax.broadcasted_iota(jnp.int32, (TOK, TOK), 0) == lax.broadcasted_iota(jnp.int32, (TOK, TOK), 1)
        bias = jnp.where(diagonal, 0.0, bias)
        yield
        contexts = []
        for g in range(2):
            q = (dot(n1, b_qkv[g, 0]).astype(BF)) * BF(HD ** -0.5)
            k = dot(n1, b_qkv[g, 1]).astype(BF)
            val = dot(n1, b_qkv[g, 2]).astype(BF)
            yield
            for pair in range(2):
                cut = slice(128 * pair, 128 * pair + 128)
                context = None
                for side in range(2):
                    inside = (pair_lane >= 64 * side) & (pair_lane < 64 * side + 64)
                    qs = jnp.where(inside, q[:, cut], BF(0))
                    vs = jnp.where(inside, val[:, cut], BF(0))
                    scores = dot_t(qs, k[:, cut]) + bias
                    top = jnp.max(scores, axis=-1, keepdims=True)
                    probs = jnp.exp2((scores - top) * LOG2E).astype(BF)
                    both = dot(probs, jnp.concatenate([vs, ones], axis=1))
                    part = both[:, :128] * (1.0 / both[:, 128:])
                    context = part if context is None else context + part
                    yield
                contexts.append(context.astype(BF))
        attended = dot(jnp.concatenate(contexts[:2], axis=1), b_proj[0])
        xone[w] = x + attended + dot(jnp.concatenate(contexts[2:], axis=1), b_proj[1])
        yield

    def finish(w):
        x1 = xone[w]
        n2 = norm(x1)
        yield
        for g in range(2):
            for c in range(2):
                h = dot(n2, b_up[g, :, 512 * c : 512 * c + 512])
                h = 0.5 * h * (1.0 + lax.erf(h * (2.0 ** -0.5)))
                hidden[:, 1024 * g + 512 * c : 1024 * g + 512 * c + 512] = h.astype(BF)
                yield
        grown = x1 + dot(hidden[:, :1024], b_down[0]) + dot(hidden[:, 1024:], b_down[1])
        yield
        n3 = norm(grown.astype(BF).astype(F32))
        yield
        by_level = dot(level[...], n3).astype(BF)
        base = jnp.zeros((64, 128), F32)
        all_kg = dot_t(b_kg[...].reshape(1024, 512), by_level)
        yield
        for g in range(2):
            kt = all_kg[256 * g : 256 * g + 256].astype(BF)
            both = dot(qbd[g], kt)
            scores = both[:64] + both[64:]
            s0, s1, s2 = scores[:, :128], scores[:, 128:256], scores[:, 256:]
            top = jnp.maximum(jnp.maximum(s0, s1), s2)
            e0, e1, e2 = (jnp.exp2((s - top) * LOG2E) for s in (s0, s1, s2))
            scale = 1.0 / (e0 + e1 + e2)
            dwt[g, 0] = e0 * scale
            dwt[g, 1] = e1 * scale
            vals = all_kg[512 + 256 * g : 768 + 256 * g]
            last_level = vals[:, 256:]
            d0, d1 = vals[:, :128] - last_level, vals[:, 128:256] - last_level
            for h in range(4):
                diff[g, h, 0] = d0[64 * h : 64 * h + 64]
                diff[g, h, 1] = d1[64 * h : 64 * h + 64]
                base = base + last_level[64 * h : 64 * h + 64]
        yield
        for l in range(NLEV):
            total = base
            for g in range(2):
                for h in range(4):
                    for j in range(2):
                        total = total + dwt[g, j, 16 * h + l : 16 * h + l + 1, :] * diff[g, h, j]
            zpix[pl.ds(l, 64, stride=16), :] = total
            if l % 4 == 3:
                yield
        packed = jnp.zeros((dests * rows, 256), F32)
        for a in range(4):
            packed = packed + dot_t(outm[a], zpix[256 * a : 256 * a + 256, :].astype(BF))
        for d in range(dests):
            for side in range(2):
                msg[w, side, d] = packed[rows * d : rows * d + rows, 128 * side : 128 * side + 128].astype(BF)
        yield

    def run(*parts):
        parts = list(parts)
        while parts:
            parts = [part for part in parts if next(part, 0) is None]

    def send(w):
        for d in range(dests):
            to = lax.rem(window_of(v, w) * dests + dests // 2 + d, grid)
            for side in range(2):
                mine = (to == me) & (v == side)

                @pl.when(mine)
                def _():
                    pltpu.make_async_copy(msg.at[w, side, d], recv.at[me], orecv).start()

                @pl.when(jnp.logical_not(mine))
                def _():
                    remote(msg.at[w, side, d], recv.at[me], osend.at[w], orecv, {"grid": to, "var": side}).start()

    first = lax.rem(me, SLOTS)
    halo(first).wait_recv()
    hear(1)
    tell(2)
    shared[0].wait()
    shared[1].wait()
    run(attend(first))
    hear(2)
    tell(3)
    for copy in shared[2:]:
        copy.wait()
    lane2 = lax.broadcasted_iota(jnp.int32, (16, 256), 1)
    for g in range(2):
        dq = b_dq[g] * (HD ** -0.5)
        for h in range(4):
            part = jnp.where((lane2 >= 64 * h) & (lane2 < 64 * h + 64), dq, 0.0)
            hi = part.astype(BF)
            qbd[g, 16 * h : 16 * h + 16, :] = hi
            qbd[g, 64 + 16 * h : 80 + 16 * h, :] = (part - hi.astype(F32)).astype(BF)


    def body(step, _):
        now, later = lax.rem(me + step, SLOTS), lax.rem(me + step + 1, SLOTS)
        halo(later).wait_recv()
        run(finish(now), attend(later))

        @pl.when(step == 0)
        def _():
            hear(3)

        send(now)
        return 0

    lax.fori_loop(0, SLOTS - 1, body, 0)
    last = lax.rem(me + SLOTS - 1, SLOTS)
    run(finish(last))
    send(last)

    my_window = lax.rem(me + grid - dests // 2, grid) // dests

    def sent(w, _):
        halo(w).wait_send()
        stays = window_of(v, w) == my_window
        row = recv.at[pl.ds(0, 2 * dests)]
        most = recv.at[pl.ds(0, 2 * dests - 1)]

        @pl.when(stays)
        def _():
            pltpu.make_async_copy(most, most, osend.at[w]).wait()

        @pl.when(jnp.logical_not(stays))
        def _():
            pltpu.make_async_copy(row, row, osend.at[w]).wait()

        return 0

    lax.fori_loop(0, SLOTS, sent, 0)
    pltpu.make_async_copy(recv, recv, orecv).wait()


def final_tables(grid):
    _, band, _ = sizes(grid)
    pad = -(-26 * band // 16) * 16
    rows = np.zeros((band, 4 * pad, 128), np.float32)
    for slot in range(band):
        for b in range(4):
            for l in range(NLEV):
                for v in range(2):
                    rows[slot, b * pad + (l * band + slot) * 2 + v, (b * 2 + v) * 16 + l] = 1
    tile = np.gcd(12 * grid, 128)
    spread = np.zeros((4, tile, 4 * tile), np.float32)
    for b in range(4):
        spread[b, np.arange(tile), 4 * np.arange(tile) + b] = 1
    return jnp.asarray(rows, BF), jnp.asarray(spread.reshape(2, 2 * tile, 4 * tile), BF)


def final_kernel(grid, recv, sel, spread, out, stage):
    _, band, _ = sizes(grid)
    cells = 12 * grid
    pad = sel.shape[1] // 4
    for s in range(grid):
        block = recv[s].astype(F32)
        start = 12 * s + 6
        for slot in range(band):
            piece = block[12 * slot : 12 * slot + 12]
            if start + 12 <= cells:
                stage[slot, start : start + 12, :] = piece
            else:
                stage[slot, start : start + 6, :] = piece[:6]
                stage[slot, 0:6, :] = piece[6:]
    flipped = jnp.zeros((4 * pad, cells), F32)
    for slot in range(band):
        flipped = flipped + dot_t(sel[slot], stage[slot].astype(BF))
    flipped = flipped.astype(BF)
    tile = spread.shape[2] // 4
    tiles = cells // tile

    def stacked(b):
        return jnp.concatenate(
            [flipped[b * pad : b * pad + pad, tile * m : tile * m + tile] for m in range(tiles)], axis=0
        )

    lines = dot(jnp.concatenate([stacked(0), stacked(1)], axis=1), spread[0]) + dot(
        jnp.concatenate([stacked(2), stacked(3)], axis=1), spread[1]
    )
    for m in range(tiles):
        for k in range(NLEV * band):
            out[k, :, 4 * tile * m : 4 * tile * (m + 1)] = lines[m * pad + 2 * k : m * pad + 2 * k + 2]


def pixels_of(grid, tokens, key_mask, w_qkv, w_proj, w_up, w_down, level_query, w_dec_q, w_dec_kv, w_dec_o, decode_matrix):
    dests, band, rows = sizes(grid)
    by_column = jnp.transpose(tokens, (1, 2, 0, 3)).reshape(36, 48, 512)
    tables = main_tables(grid)
    operands = (
        by_column, key_mask.T, w_qkv, w_proj, w_up, w_down, level_query, w_dec_q, w_dec_kv, w_dec_o, decode_matrix.T,
    ) + tables
    vm = pltpu.VMEM
    return pl.pallas_call(
        functools.partial(main_kernel, grid),
        out_shape=jax.ShapeDtypeStruct((grid, rows, 128), BF),
        in_specs=[pl.BlockSpec(memory_space=pltpu.HBM)] * len(operands),
        out_specs=pl.BlockSpec(memory_space=pl.ANY),
        scratch_shapes=[
            vm((36, 48, 512), BF),
            vm((SLOTS, HALF, 512), BF),
            vm((SLOTS, HALF, 512), BF),
            vm((SLOTS, HALF, 512), BF),
            vm((SLOTS, TOK, 512), F32),
            vm((2, 3, 512, 256), BF),
            vm((2, 256, 512), BF),
            vm((2, 512, 1024), BF),
            vm((2, 1024, 512), BF),
            vm((4, 256, 512), BF),
            vm((2, 16, 256), F32),
            vm((2, 128, 256), BF),
            vm((13, 512), BF),
            vm((512, 256), BF),
            vm((2, 512, 256), BF),
            vm((256, 512), BF),
            vm((64, 512), F32),
            *[vm(table.shape[1:] if i < 2 else table.shape, table.dtype) for i, table in enumerate(tables)],
            vm((12, 48), jnp.int32),
            vm((12, 48), jnp.int32),
            vm((32, 48), F32),
            vm((TOK, 2048), BF),
            vm((2, 4, 2, 64, 128), F32),
            vm((2, 2, 64, 128), F32),
            vm((1024, 128), F32),
            vm((SLOTS, 2, dests, rows, 128), BF),
            pltpu.SemaphoreType.DMA((20,)),
            pltpu.SemaphoreType.DMA((7,)),
            pltpu.SemaphoreType.DMA((7,)),
            pltpu.SemaphoreType.DMA((SLOTS + 1,)),
            pltpu.SemaphoreType.DMA((SLOTS + 1,)),
            pltpu.SemaphoreType.DMA((SLOTS,)),
            pltpu.SemaphoreType.DMA,
            pltpu.SemaphoreType.REGULAR((4,)),
        ],
        compiler_params=pltpu.CompilerParams(
            collective_id=0, has_side_effects=True, vmem_limit_bytes=60 * 2**20
        ),
    )(*operands)


def assemble(grid, received):
    _, band, _ = sizes(grid)
    tables = final_tables(grid)
    lines = pl.pallas_call(
        functools.partial(final_kernel, grid),
        out_shape=jax.ShapeDtypeStruct((NLEV * band, 2, 48 * grid), F32),
        scratch_shapes=[pltpu.VMEM((band, 12 * grid, 128), F32)],
        compiler_params=pltpu.CompilerParams(vmem_limit_bytes=32 * 2**20),
    )(received, *tables)
    return jnp.transpose(lines.reshape(NLEV, band, 2, 48 * grid), (2, 0, 1, 3))


def local(*args):
    grid = lax.axis_size("grid")
    return assemble(grid, pixels_of(grid, *args))


def solution(mesh):
    placed = (
        P("group", "grid", None, None),
        P("group", "grid"),
        P(None, None, "var"),
        P("var", None),
        P(None, "var"),
        P("var", None),
        P(),
        P(None, "var"),
        P(None, None, "var"),
        P("var", None),
        P(),
    )
    return jax.shard_map(
        local, mesh=mesh, in_specs=placed, out_specs=P("var", "group", "grid", None), check_vma=False
    )
```

```python
import functools

import jax
import jax.numpy as jnp
import numpy as np
from jax import lax
from jax.experimental import pallas as pl
from jax.experimental.pallas import tpu as pltpu
from jax.sharding import PartitionSpec as P

HD = 64
WIN = 6
LEV = 3
PIX = 4
NLEV = 13
HALF = 112
TOK = 2 * HALF
EPSILON = 1e-05
LOG2E = 1.4426950408889634
NEG = -1e30
BF = jnp.bfloat16
F32 = jnp.float32


SLOTS = 4


def window_of(v, slot):
    return (7 * v + 2 * slot) % 8


def sizes(grid):
    dests = grid // 8
    band = WIN * PIX // dests
    rows = -(-(band * 12) // 8) * 8
    return dests, band, rows


def reach(grid):
    stride = int(round(grid**0.5)) if grid > 8 else 2
    radius = 0
    for k in range(grid):
        ways = [abs(b) + min((k - stride * b) % grid, (stride * b - k) % grid) for b in range(-stride, stride + 1)]
        radius = max(radius, min(ways))
    rounds = max(0, (radius - 1).bit_length())
    assert rounds <= 3
    return stride, rounds


def token_fields():
    t = np.arange(TOK)
    half, q = t // HALF, t % HALF
    valid = q < 108
    cj, r = q // 6, q % 6
    return half, cj // 3, cj % 3, r, valid


def main_tables(grid):
    dests, band, rows = sizes(grid)
    pick = np.zeros((2, SLOTS * 48, 8 * 48), np.float32)
    pick2 = np.zeros((2, SLOTS * 16, 2 * 48), np.float32)
    for v in range(2):
        for step in range(SLOTS):
            for r in range(6):
                row = (6 * int(window_of(v, step)) + 3 + r) % 48
                for cj in range(8):
                    pick[v, step * 48 + cj * 6 + r, cj * 48 + row] = 1
                for cj in range(2):
                    pick2[v, step * 16 + cj * 6 + r, cj * 48 + row] = 1
    half, c6, j, r, valid = token_fields()
    level_rows = np.zeros((384, TOK), np.float32)
    t = np.arange(TOK)[valid]
    patch = half * 36 + c6 * 6 + r
    level_rows[j[valid] * 128 + patch[valid], t] = 1
    out_rows = np.zeros((4, dests * rows, 128), np.float32)
    for d in range(dests):
        for slot in range(band):
            rr, a = divmod(band * d + slot, 4)
            for c in range(12):
                out_rows[a, d * rows + slot * 12 + c, (c // 6) * 36 + (c % 6) * 6 + rr] = 1
    mask_rows = np.zeros((8, 48, TOK), np.float32)
    for window in range(8):
        mask_rows[window, ((6 * window + 3 + r) % 48)[valid], t] = 1
    mask_cols = np.zeros((32, TOK), np.float32)
    mask_cols[np.where(half == 0, 6 + c6, 16 + c6)[valid], t] = 1
    seam = np.where((r >= 3)[:, None] == (r >= 3)[None, :], 0, NEG).astype(np.float32)
    order = np.zeros((64, 64), np.float32)
    for a in range(4):
        for vh in range(2):
            for b in range(4):
                for v in range(2):
                    order[((a * 2 + vh) * 4 + b) * 2 + v, ((vh * 2 + v) * 4 + a) * 4 + b] = 1
    return (
        jnp.asarray(pick, BF),
        jnp.asarray(pick2, BF),
        jnp.asarray(level_rows, BF),
        jnp.asarray(out_rows, BF),
        jnp.asarray(mask_rows, BF),
        jnp.asarray(mask_cols, F32),
        jnp.asarray(seam, F32),
        jnp.asarray(order, BF),
    )


def dot(a, b):
    return lax.dot_general(a, b, (((1,), (0,)), ((), ())), preferred_element_type=F32)


def dot_t(a, b):
    return lax.dot_general(a, b, (((1,), (1,)), ((), ())), preferred_element_type=F32)


def norm(values):
    center = values - jnp.mean(values, axis=-1, keepdims=True)
    spread = jnp.mean(center * center, axis=-1, keepdims=True)
    return (center * lax.rsqrt(spread + EPSILON)).astype(BF)


def split3(values):
    hi = values.astype(BF)
    rest = values - hi.astype(F32)
    mid = rest.astype(BF)
    return hi, mid, (rest - mid.astype(F32)).astype(BF)


def main_kernel(
    grid,
    tokens, mask, w_qkv, w_proj, w_up, w_down, query, w_dec_q, w_dec_kv, w_dec_o, decode_t,
    c_pick, c_pick2, c_level, c_out, c_mrow, c_mcol, c_seam, c_order,
    recv,
    tok, own, hsend, hrecv, xone, normed, b_qkv, b_proj, b_up, b_down, b_kg, b_dq, qbd,
    v_query, v_dq, v_dkv, v_do, v_dec, pick, pick2, level, outm, mrow, mcol, seam, order,
    mask_own, mask_right, marks, hidden, diff, dwt, zpix, msg,
    lsem, wsend, wrecv, hssem, hrsem, osend, orecv, heard,
):
    dests, band, rows = sizes(grid)
    assert grid & (grid - 1) == 0
    me = lax.axis_index("grid")
    v = lax.axis_index("var")
    partner = {"var": 1 - v}
    west = {"grid": lax.rem(me + grid - 1, grid)}

    barrier = pltpu.get_barrier_semaphore()

    def signal(sem, where):
        pl.semaphore_signal(sem, inc=1, device_id=where, device_id_type=pl.DeviceIdType.MESH)

    stride, rounds = reach(grid)
    sides = (1, grid - 1, stride, grid - stride)
    signal(barrier, partner)
    for by in sides:
        signal(barrier, {"grid": lax.rem(me + by, grid)})

    def tell(k):
        if k < rounds:
            for by in sides:
                signal(heard.at[k], {"grid": lax.rem(me + by * 2**k, grid)})
        elif k == rounds:
            signal(heard.at[k], partner)

    def hear(k):
        if k <= rounds:
            pl.semaphore_wait(heard.at[k], 4 if k < rounds else 1)

    loads = [
        (tokens.at[pl.ds(0, 18)], tok.at[pl.ds(0, 18)]),
        (c_pick.at[v], pick),
        (c_pick2.at[v], pick2),
        (tokens.at[pl.ds(18, 18)], tok.at[pl.ds(18, 18)]),
        (w_dec_o, v_do),
        (decode_t, v_dec),
        (c_order, order),
        (w_dec_kv, v_dkv),
        (query, v_query),
        (w_dec_q, v_dq),
        (mask, mask_own),
        (w_qkv, b_qkv.at[v]),
        (c_mrow, mrow),
        (c_mcol, mcol),
        (c_seam, seam),
        (w_proj, b_proj.at[v]),
        (w_up, b_up.at[v]),
        (w_down, b_down.at[v]),
        (c_level, level),
        (c_out, outm),
    ]
    local = [pltpu.make_async_copy(src, dst, lsem.at[i]) for i, (src, dst) in enumerate(loads)]
    for copy in local:
        copy.start()

    def remote(src, dst, send, recv_sem, where):
        return pltpu.make_async_remote_copy(
            src_ref=src, dst_ref=dst, send_sem=send, recv_sem=recv_sem, device_id=where, device_id_type=pl.DeviceIdType.MESH
        )

    def halo(w):
        return remote(hsend.at[w], hrecv.at[w], hssem.at[w], hrsem.at[w], west)

    weights = [
        (w_qkv, b_qkv.at[v]),
        (w_proj, b_proj.at[v]),
        (w_up, b_up.at[v]),
        (w_down, b_down.at[v]),
        (b_kg.at[v], b_kg.at[v]),
        (b_kg.at[2 + v], b_kg.at[2 + v]),
        (b_dq.at[v], b_dq.at[v]),
    ]
    shared = [remote(src, dst, wsend.at[i], wrecv.at[i], partner) for i, (src, dst) in enumerate(weights)]
    mask_copy = remote(mask, mask_right, hssem.at[SLOTS], hrsem.at[SLOTS], west)

    def pack(part, target):
        for block in range(2):
            src = tok[part + 8 * block : part + 8 * block + 8].reshape(384, 512)
            packed = dot(pick[...], src).astype(BF)
            for w in range(SLOTS):
                target[w, 48 * block : 48 * block + 48, :] = packed[48 * w : 48 * w + 48]
        src = tok[part + 16 : part + 18].reshape(96, 512)
        packed = dot(pick2[...], src).astype(BF)
        for w in range(SLOTS):
            target[w, 96:112, :] = packed[16 * w : 16 * w + 16]

    pl.semaphore_wait(barrier, 5)
    for copy in shared[:4]:
        copy.start()
    mask_copy.start()
    tell(0)

    for i in range(3):
        local[i].wait()
    pack(0, hsend)
    def send_halo(step):
        halo(lax.rem(me + grid - 1 + step, SLOTS)).start()

    send_halo(0)
    local[3].wait()
    pack(18, own)

    for i in range(4, 10):
        local[i].wait()
    dec = v_dec[...]
    hi, mid, low = split3(dec)
    do = v_do[...]
    unembed = (dot_t(hi, do) + dot_t(mid, do) + dot_t(low, do)).astype(BF)
    unembed = dot(order[...], unembed).astype(BF)
    lane = lax.broadcasted_iota(jnp.int32, (64, 256), 1)
    for h in range(4):
        block = jnp.where((lane >= 64 * h) & (lane < 64 * h + 64), unembed.astype(F32), 0).astype(BF)
        b_kg[2 + v, 64 * h : 64 * h + 64, :] = dot_t(block, v_dkv[1]).astype(BF)
    eye = jnp.where(
        lax.broadcasted_iota(jnp.int32, (256, 256), 0) == lax.broadcasted_iota(jnp.int32, (256, 256), 1), 1.0, 0.0
    ).astype(BF)
    b_kg[v] = dot_t(eye, v_dkv[0]).astype(BF)
    b_dq[v, 0:13, :] = dot(v_query[...], v_dq[...])
    b_dq[v, 13:16, :] = jnp.zeros((3, 256), F32)

    for copy in shared[4:]:
        copy.start()
    send_halo(1)
    hear(0)
    tell(1)
    zpix[...] = jnp.zeros_like(zpix)
    marks[...] = jnp.zeros_like(marks)

    for i in range(10, len(local)):
        local[i].wait()
    mask_copy.wait()
    marks[0:12, :] = mask_own[...].astype(F32)
    marks[16:28, :] = mask_right[...].astype(F32)
    pair_lane = lax.broadcasted_iota(jnp.int32, (TOK, 128), 1)
    ones = jnp.ones((TOK, 128), BF)

    def attend(w):
        which = window_of(v, w)
        x = jnp.concatenate([own[w], hrecv[w]], axis=0).astype(F32)
        n1 = norm(x)
        kept = jnp.sum(dot(marks[...].astype(BF), mrow[which]) * mcol[...], axis=0, keepdims=True)
        last = jnp.where(which == 7, 1.0, 0.0)
        bias = seam[...] * last + jnp.where(kept > 0.5, 0.0, NEG)
        diagonal = lax.broadcasted_iota(jnp.int32, (TOK, TOK), 0) == lax.broadcasted_iota(jnp.int32, (TOK, TOK), 1)
        bias = jnp.where(diagonal, 0.0, bias)
        yield
        contexts = []

        def head(scores, vs):
            top = jnp.max(scores, axis=-1, keepdims=True)
            probs = jnp.exp2((scores - top) * LOG2E).astype(BF)
            both = dot(probs, jnp.concatenate([vs, ones], axis=1))
            contexts.append(both[:, :128] * (1.0 / both[:, 128:]))

        waiting = None
        for g in range(2):
            q = (dot(n1, b_qkv[g, 0]).astype(BF)) * BF(HD ** -0.5)
            k = dot(n1, b_qkv[g, 1]).astype(BF)
            val = dot(n1, b_qkv[g, 2]).astype(BF)
            yield
            for pair in range(2):
                cut = slice(128 * pair, 128 * pair + 128)
                for side in range(2):
                    inside = (pair_lane >= 64 * side) & (pair_lane < 64 * side + 64)
                    qs = jnp.where(inside, q[:, cut], BF(0))
                    vs = jnp.where(inside, val[:, cut], BF(0))
                    scores = dot_t(qs, k[:, cut]) + bias
                    if waiting is not None:
                        head(*waiting)
                    waiting = scores, vs
                    yield
        head(*waiting)
        contexts = [(contexts[2 * i] + contexts[2 * i + 1]).astype(BF) for i in range(4)]
        attended = dot(jnp.concatenate(contexts[:2], axis=1), b_proj[0])
        x1 = x + attended + dot(jnp.concatenate(contexts[2:], axis=1), b_proj[1])
        xone[w] = x1
        normed[w] = norm(x1)
        yield

    def finish(w):
        n2 = normed[w]
        for g in range(2):
            for c in range(2):
                h = dot(n2, b_up[g, :, 512 * c : 512 * c + 512])
                h = 0.5 * h * (1.0 + lax.erf(h * (2.0 ** -0.5)))
                hidden[:, 1024 * g + 512 * c : 1024 * g + 512 * c + 512] = h.astype(BF)
                yield
        grown = xone[w] + dot(hidden[:, :1024], b_down[0]) + dot(hidden[:, 1024:], b_down[1])
        yield
        n3 = norm(grown.astype(BF).astype(F32))
        yield
        by_level = dot(level[...], n3).astype(BF)
        base = jnp.zeros((64, 128), F32)
        all_kg = dot_t(b_kg[...].reshape(1024, 512), by_level)
        yield
        for g in range(2):
            kt = all_kg[256 * g : 256 * g + 256].astype(BF)
            both = dot(qbd[g], kt)
            scores = both[:64] + both[64:]
            s0, s1, s2 = scores[:, :128], scores[:, 128:256], scores[:, 256:]
            top = jnp.maximum(jnp.maximum(s0, s1), s2)
            e0, e1, e2 = (jnp.exp2((s - top) * LOG2E) for s in (s0, s1, s2))
            scale = 1.0 / (e0 + e1 + e2)
            dwt[g, 0] = e0 * scale
            dwt[g, 1] = e1 * scale
            vals = all_kg[512 + 256 * g : 768 + 256 * g]
            last_level = vals[:, 256:]
            d0, d1 = vals[:, :128] - last_level, vals[:, 128:256] - last_level
            for h in range(4):
                diff[g, h, 0] = d0[64 * h : 64 * h + 64]
                diff[g, h, 1] = d1[64 * h : 64 * h + 64]
                base = base + last_level[64 * h : 64 * h + 64]
        yield
        for group in ((0, 1, 2, 3), (4, 5, 6, 7), (8, 9, 10, 11, 12)):
            totals = [base] * len(group)
            for g in range(2):
                for h in range(4):
                    for j in range(2):
                        step = diff[g, h, j]
                        totals = [
                            total + dwt[g, j, 16 * h + l : 16 * h + l + 1, :] * step for total, l in zip(totals, group)
                        ]
            for total, l in zip(totals, group):
                zpix[pl.ds(l, 64, stride=16), :] = total
            yield
        packed = jnp.zeros((dests * rows, 256), F32)
        for a in range(4):
            packed = packed + dot_t(outm[a], zpix[256 * a : 256 * a + 256, :].astype(BF))
        for d in range(dests):
            for side in range(2):
                msg[w, side, d] = packed[rows * d : rows * d + rows, 128 * side : 128 * side + 128].astype(BF)
        yield

    def run(*parts, order=""):
        for which in order:
            next(parts[int(which)], None)
        for part in parts:
            for _ in part:
                pass

    my_window = lax.rem(me + grid - dests // 2, grid) // dests

    def send(w):
        base = window_of(v, w) * dests + dests // 2
        stays = window_of(v, w) == my_window

        def one(d, side, to):
            return remote(msg.at[w, side, d], recv.at[me], osend.at[w], orecv, {"grid": to, "var": side})

        for d in range(dests):
            to = (base + d) & (grid - 1)
            one(d, 1 - v, to).start()

            @pl.when(jnp.logical_not(stays & (to == me)))
            def _():
                one(d, v, to).start()

        @pl.when(stays)
        def _():
            d = (me - base) & (grid - 1)
            pltpu.make_async_copy(msg.at[w, v, d], recv.at[me], orecv).start()

    first = lax.rem(me, SLOTS)
    halo(first).wait_recv()
    send_halo(2)
    send_halo(3)
    shared[0].wait()
    shared[1].wait()
    run(attend(first))
    hear(1)
    tell(2)
    for copy in shared[2:]:
        copy.wait()
    lane2 = lax.broadcasted_iota(jnp.int32, (16, 256), 1)
    for g in range(2):
        dq = b_dq[g] * (HD ** -0.5)
        for h in range(4):
            part = jnp.where((lane2 >= 64 * h) & (lane2 < 64 * h + 64), dq, 0.0)
            hi = part.astype(BF)
            qbd[g, 16 * h : 16 * h + 16, :] = hi
            qbd[g, 64 + 16 * h : 80 + 16 * h, :] = (part - hi.astype(F32)).astype(BF)


    def body(step, _):
        now, later = lax.rem(me + step, SLOTS), lax.rem(me + step + 1, SLOTS)
        halo(later).wait_recv()
        run(finish(now), attend(later), order="10000010110101101101101")

        @pl.when(step == 0)
        def _():
            hear(2)
            tell(3)
            hear(3)

        send(now)
        return 0

    lax.fori_loop(0, SLOTS - 1, body, 0)
    last = lax.rem(me + SLOTS - 1, SLOTS)
    run(finish(last))
    send(last)

    def sent(w, _):
        halo(w).wait_send()
        stays = window_of(v, w) == my_window
        row = recv.at[pl.ds(0, 2 * dests)]
        most = recv.at[pl.ds(0, 2 * dests - 1)]

        @pl.when(stays)
        def _():
            pltpu.make_async_copy(most, most, osend.at[w]).wait()

        @pl.when(jnp.logical_not(stays))
        def _():
            pltpu.make_async_copy(row, row, osend.at[w]).wait()

        return 0

    lax.fori_loop(0, SLOTS, sent, 0)
    pltpu.make_async_copy(recv, recv, orecv).wait()


def final_tables(grid):
    _, band, _ = sizes(grid)
    pad = -(-26 * band // 16) * 16
    rows = np.zeros((band, 4 * pad, 128), np.float32)
    for slot in range(band):
        for b in range(4):
            for l in range(NLEV):
                for v in range(2):
                    rows[slot, b * pad + (l * band + slot) * 2 + v, (b * 2 + v) * 16 + l] = 1
    tile = np.gcd(12 * grid, 128)
    spread = np.zeros((4, tile, 4 * tile), np.float32)
    for b in range(4):
        spread[b, np.arange(tile), 4 * np.arange(tile) + b] = 1
    return jnp.asarray(rows, BF), jnp.asarray(spread.reshape(2, 2 * tile, 4 * tile), BF)


def final_kernel(grid, recv, sel, spread, out, stage):
    _, band, _ = sizes(grid)
    cells = 12 * grid
    pad = sel.shape[1] // 4
    for s in range(grid):
        block = recv[s].astype(F32)
        start = 12 * s + 6
        for slot in range(band):
            piece = block[12 * slot : 12 * slot + 12]
            if start + 12 <= cells:
                stage[slot, start : start + 12, :] = piece
            else:
                stage[slot, start : start + 6, :] = piece[:6]
                stage[slot, 0:6, :] = piece[6:]
    flipped = jnp.zeros((4 * pad, cells), F32)
    for slot in range(band):
        flipped = flipped + dot_t(sel[slot], stage[slot].astype(BF))
    flipped = flipped.astype(BF)
    tile = spread.shape[2] // 4
    tiles = cells // tile

    def stacked(b):
        return jnp.concatenate(
            [flipped[b * pad : b * pad + pad, tile * m : tile * m + tile] for m in range(tiles)], axis=0
        )

    lines = dot(jnp.concatenate([stacked(0), stacked(1)], axis=1), spread[0]) + dot(
        jnp.concatenate([stacked(2), stacked(3)], axis=1), spread[1]
    )
    for m in range(tiles):
        for k in range(NLEV * band):
            out[k, :, 4 * tile * m : 4 * tile * (m + 1)] = lines[m * pad + 2 * k : m * pad + 2 * k + 2]


def pixels_of(grid, tokens, key_mask, w_qkv, w_proj, w_up, w_down, level_query, w_dec_q, w_dec_kv, w_dec_o, decode_matrix):
    dests, band, rows = sizes(grid)
    by_column = jnp.transpose(tokens, (1, 2, 0, 3)).reshape(36, 48, 512)
    tables = main_tables(grid)
    operands = (
        by_column, key_mask.T, w_qkv, w_proj, w_up, w_down, level_query, w_dec_q, w_dec_kv, w_dec_o, decode_matrix.T,
    ) + tables
    vm = pltpu.VMEM
    return pl.pallas_call(
        functools.partial(main_kernel, grid),
        out_shape=pltpu.VMEM((grid, rows, 128), BF),
        in_specs=[pl.BlockSpec(memory_space=pltpu.HBM)] * len(operands),
        out_specs=pl.BlockSpec(memory_space=pltpu.VMEM),
        scratch_shapes=[
            vm((36, 48, 512), BF),
            vm((SLOTS, HALF, 512), BF),
            vm((SLOTS, HALF, 512), BF),
            vm((SLOTS, HALF, 512), BF),
            vm((SLOTS, TOK, 512), F32),
            vm((SLOTS, TOK, 512), BF),
            vm((2, 3, 512, 256), BF),
            vm((2, 256, 512), BF),
            vm((2, 512, 1024), BF),
            vm((2, 1024, 512), BF),
            vm((4, 256, 512), BF),
            vm((2, 16, 256), F32),
            vm((2, 128, 256), BF),
            vm((13, 512), BF),
            vm((512, 256), BF),
            vm((2, 512, 256), BF),
            vm((256, 512), BF),
            vm((64, 512), F32),
            *[vm(table.shape[1:] if i < 2 else table.shape, table.dtype) for i, table in enumerate(tables)],
            vm((12, 48), jnp.int32),
            vm((12, 48), jnp.int32),
            vm((32, 48), F32),
            vm((TOK, 2048), BF),
            vm((2, 4, 2, 64, 128), F32),
            vm((2, 2, 64, 128), F32),
            vm((1024, 128), F32),
            vm((SLOTS, 2, dests, rows, 128), BF),
            pltpu.SemaphoreType.DMA((20,)),
            pltpu.SemaphoreType.DMA((7,)),
            pltpu.SemaphoreType.DMA((7,)),
            pltpu.SemaphoreType.DMA((SLOTS + 1,)),
            pltpu.SemaphoreType.DMA((SLOTS + 1,)),
            pltpu.SemaphoreType.DMA((SLOTS,)),
            pltpu.SemaphoreType.DMA,
            pltpu.SemaphoreType.REGULAR((4,)),
        ],
        compiler_params=pltpu.CompilerParams(
            collective_id=0, has_side_effects=True, vmem_limit_bytes=60 * 2**20
        ),
    )(*operands)


def assemble(grid, received):
    _, band, _ = sizes(grid)
    tables = final_tables(grid)
    lines = pl.pallas_call(
        functools.partial(final_kernel, grid),
        in_specs=[pl.BlockSpec(memory_space=pltpu.VMEM)] * 3,
        out_shape=jax.ShapeDtypeStruct((NLEV * band, 2, 48 * grid), F32),
        scratch_shapes=[pltpu.VMEM((band, 12 * grid, 128), F32)],
        compiler_params=pltpu.CompilerParams(vmem_limit_bytes=32 * 2**20),
    )(received, *tables)
    return jnp.transpose(lines.reshape(NLEV, band, 2, 48 * grid), (2, 0, 1, 3))


def local(*args):
    grid = lax.axis_size("grid")
    return assemble(grid, pixels_of(grid, *args))


def solution(mesh):
    placed = (
        P("group", "grid", None, None),
        P("group", "grid"),
        P(None, None, "var"),
        P("var", None),
        P(None, "var"),
        P("var", None),
        P(),
        P(None, "var"),
        P(None, None, "var"),
        P("var", None),
        P(),
    )
    return jax.shard_map(
        local, mesh=mesh, in_specs=placed, out_specs=P("var", "group", "grid", None), check_vma=False
    )
```

```python
import functools

import jax
import jax.numpy as jnp
import numpy as np
from jax import lax
from jax.experimental import pallas as pl
from jax.experimental.pallas import tpu as pltpu
from jax.sharding import PartitionSpec as P

HD = 64
WIN = 6
LEV = 3
PIX = 4
NLEV = 13
HALF = 112
TOK = 2 * HALF
EPSILON = 1e-05
LOG2E = 1.4426950408889634
NEG = -1e30
BF = jnp.bfloat16
F32 = jnp.float32


SLOTS = 4


def window_of(v, slot):
    return (7 * v + 2 * slot) % 8


def sizes(grid):
    dests = grid // 8
    band = WIN * PIX // dests
    rows = -(-(band * 12) // 8) * 8
    return dests, band, rows


def reach(grid):
    stride = int(round(grid**0.5)) if grid > 8 else 2
    radius = 0
    for k in range(grid):
        ways = [abs(b) + min((k - stride * b) % grid, (stride * b - k) % grid) for b in range(-stride, stride + 1)]
        radius = max(radius, min(ways))
    rounds = max(0, (radius - 1).bit_length())
    assert rounds <= 3
    return stride, rounds


def token_fields():
    t = np.arange(TOK)
    half, q = t // HALF, t % HALF
    valid = q < 108
    cj, r = q // 6, q % 6
    return half, cj // 3, cj % 3, r, valid


def main_tables(grid):
    dests, band, rows = sizes(grid)
    pick = np.zeros((2, SLOTS * 48, 8 * 48), np.float32)
    pick2 = np.zeros((2, SLOTS * 16, 2 * 48), np.float32)
    for v in range(2):
        for step in range(SLOTS):
            for r in range(6):
                row = (6 * int(window_of(v, step)) + 3 + r) % 48
                for cj in range(8):
                    pick[v, step * 48 + cj * 6 + r, cj * 48 + row] = 1
                for cj in range(2):
                    pick2[v, step * 16 + cj * 6 + r, cj * 48 + row] = 1
    half, c6, j, r, valid = token_fields()
    level_rows = np.zeros((384, TOK), np.float32)
    t = np.arange(TOK)[valid]
    patch = half * 36 + c6 * 6 + r
    level_rows[j[valid] * 128 + patch[valid], t] = 1
    out_rows = np.zeros((4, dests * rows, 128), np.float32)
    for d in range(dests):
        for slot in range(band):
            rr, a = divmod(band * d + slot, 4)
            for c in range(12):
                out_rows[a, d * rows + slot * 12 + c, (c // 6) * 36 + (c % 6) * 6 + rr] = 1
    mask_rows = np.zeros((8, 48, TOK), np.float32)
    for window in range(8):
        mask_rows[window, ((6 * window + 3 + r) % 48)[valid], t] = 1
    mask_cols = np.zeros((32, TOK), np.float32)
    mask_cols[np.where(half == 0, 6 + c6, 16 + c6)[valid], t] = 1
    seam = np.where((r >= 3)[:, None] == (r >= 3)[None, :], 0, NEG).astype(np.float32)
    order = np.zeros((64, 64), np.float32)
    for a in range(4):
        for vh in range(2):
            for b in range(4):
                for v in range(2):
                    order[((a * 2 + vh) * 4 + b) * 2 + v, ((vh * 2 + v) * 4 + a) * 4 + b] = 1
    return (
        jnp.asarray(pick, BF),
        jnp.asarray(pick2, BF),
        jnp.asarray(level_rows, BF),
        jnp.asarray(out_rows, BF),
        jnp.asarray(mask_rows, BF),
        jnp.asarray(mask_cols, F32),
        jnp.asarray(seam, F32),
        jnp.asarray(order, BF),
    )


def dot(a, b):
    return lax.dot_general(a, b, (((1,), (0,)), ((), ())), preferred_element_type=F32)


def dot_t(a, b):
    return lax.dot_general(a, b, (((1,), (1,)), ((), ())), preferred_element_type=F32)


def norm(values):
    center = values - jnp.mean(values, axis=-1, keepdims=True)
    spread = jnp.mean(center * center, axis=-1, keepdims=True)
    return (center * lax.rsqrt(spread + EPSILON)).astype(BF)


def split3(values):
    hi = values.astype(BF)
    rest = values - hi.astype(F32)
    mid = rest.astype(BF)
    return hi, mid, (rest - mid.astype(F32)).astype(BF)


def main_kernel(
    grid,
    tokens, mask, w_qkv, w_proj, w_up, w_down, query, w_dec_q, w_dec_kv, w_dec_o, decode_t,
    c_pick, c_pick2, c_level, c_out, c_mrow, c_mcol, c_seam, c_order,
    recv,
    tok, own, hsend, hrecv, xone, normed, b_qkv, b_proj, b_up, b_down, b_kg, b_dq, qbd,
    v_query, v_dq, v_dkv, v_do, v_dec, pick, pick2, level, outm, mrow, mcol, seam, order,
    mask_own, mask_right, marks, hidden, diff, dwt, zpix, msg,
    lsem, wsend, wrecv, hssem, hrsem, osend, orecv, heard,
):
    dests, band, rows = sizes(grid)
    assert grid & (grid - 1) == 0
    me = lax.axis_index("grid")
    v = lax.axis_index("var")
    partner = {"var": 1 - v}
    west = {"grid": lax.rem(me + grid - 1, grid)}

    barrier = pltpu.get_barrier_semaphore()

    def signal(sem, where):
        pl.semaphore_signal(sem, inc=1, device_id=where, device_id_type=pl.DeviceIdType.MESH)

    stride, rounds = reach(grid)
    sides = (1, grid - 1, stride, grid - stride)
    signal(barrier, partner)
    for by in sides:
        signal(barrier, {"grid": lax.rem(me + by, grid)})

    def tell(k):
        if k < rounds:
            for by in sides:
                signal(heard.at[k], {"grid": lax.rem(me + by * 2**k, grid)})
        elif k == rounds:
            signal(heard.at[k], partner)

    def hear(k):
        if k <= rounds:
            pl.semaphore_wait(heard.at[k], 4 if k < rounds else 1)

    loads = [
        (tokens.at[pl.ds(0, 18)], tok.at[pl.ds(0, 18)]),
        (c_pick.at[v], pick),
        (c_pick2.at[v], pick2),
        (tokens.at[pl.ds(18, 18)], tok.at[pl.ds(18, 18)]),
        (w_dec_o, v_do),
        (decode_t, v_dec),
        (c_order, order),
        (w_dec_kv, v_dkv),
        (query, v_query),
        (w_dec_q, v_dq),
        (mask, mask_own),
        (w_qkv, b_qkv.at[v]),
        (c_mrow, mrow),
        (c_mcol, mcol),
        (c_seam, seam),
        (w_proj, b_proj.at[v]),
        (w_up, b_up.at[v]),
        (w_down, b_down.at[v]),
        (c_level, level),
        (c_out, outm),
    ]
    local = [pltpu.make_async_copy(src, dst, lsem.at[i]) for i, (src, dst) in enumerate(loads)]
    for copy in local:
        copy.start()

    def remote(src, dst, send, recv_sem, where):
        return pltpu.make_async_remote_copy(
            src_ref=src, dst_ref=dst, send_sem=send, recv_sem=recv_sem, device_id=where, device_id_type=pl.DeviceIdType.MESH
        )

    def halo(w):
        return remote(hsend.at[w], hrecv.at[w], hssem.at[w], hrsem.at[w], west)

    weights = [
        (w_qkv, b_qkv.at[v]),
        (w_proj, b_proj.at[v]),
        (w_up, b_up.at[v]),
        (w_down, b_down.at[v]),
        (b_kg.at[v], b_kg.at[v]),
        (b_kg.at[2 + v], b_kg.at[2 + v]),
        (b_dq.at[v], b_dq.at[v]),
    ]
    shared = [remote(src, dst, wsend.at[i], wrecv.at[i], partner) for i, (src, dst) in enumerate(weights)]
    mask_copy = remote(mask, mask_right, hssem.at[SLOTS], hrsem.at[SLOTS], west)

    def pack(part, target):
        for block in range(2):
            src = tok[part + 8 * block : part + 8 * block + 8].reshape(384, 512)
            packed = dot(pick[...], src).astype(BF)
            for w in range(SLOTS):
                target[w, 48 * block : 48 * block + 48, :] = packed[48 * w : 48 * w + 48]
        src = tok[part + 16 : part + 18].reshape(96, 512)
        packed = dot(pick2[...], src).astype(BF)
        for w in range(SLOTS):
            target[w, 96:112, :] = packed[16 * w : 16 * w + 16]

    def send_halo(step):
        halo(lax.rem(me + grid - 1 + step, SLOTS)).start()

    for i in range(3):
        local[i].wait()
    pack(0, hsend)
    pl.semaphore_wait(barrier, 5)
    tell(0)
    mask_copy.start()
    send_halo(0)
    shared[0].start()
    shared[1].start()
    send_halo(1)
    shared[2].start()
    send_halo(2)
    shared[3].start()
    send_halo(3)
    local[3].wait()
    pack(18, own)

    for i in range(4, 10):
        local[i].wait()
    dec = v_dec[...]
    hi, mid, low = split3(dec)
    do = v_do[...]
    unembed = (dot_t(hi, do) + dot_t(mid, do) + dot_t(low, do)).astype(BF)
    unembed = dot(order[...], unembed).astype(BF)
    lane = lax.broadcasted_iota(jnp.int32, (64, 256), 1)
    for h in range(4):
        block = jnp.where((lane >= 64 * h) & (lane < 64 * h + 64), unembed.astype(F32), 0).astype(BF)
        b_kg[2 + v, 64 * h : 64 * h + 64, :] = dot_t(block, v_dkv[1]).astype(BF)
    eye = jnp.where(
        lax.broadcasted_iota(jnp.int32, (256, 256), 0) == lax.broadcasted_iota(jnp.int32, (256, 256), 1), 1.0, 0.0
    ).astype(BF)
    b_kg[v] = dot_t(eye, v_dkv[0]).astype(BF)
    b_dq[v, 0:13, :] = dot(v_query[...], v_dq[...])
    b_dq[v, 13:16, :] = jnp.zeros((3, 256), F32)

    for copy in shared[4:]:
        copy.start()
    hear(0)
    tell(1)
    zpix[...] = jnp.zeros_like(zpix)
    marks[...] = jnp.zeros_like(marks)

    for i in range(10, len(local)):
        local[i].wait()
    mask_copy.wait()
    marks[0:12, :] = mask_own[...].astype(F32)
    marks[16:28, :] = mask_right[...].astype(F32)
    pair_lane = lax.broadcasted_iota(jnp.int32, (TOK, 128), 1)
    ones = jnp.ones((TOK, 128), BF)

    def attend(w):
        which = window_of(v, w)
        x = jnp.concatenate([own[w], hrecv[w]], axis=0).astype(F32)
        n1 = norm(x)
        kept = jnp.sum(dot(marks[...].astype(BF), mrow[which]) * mcol[...], axis=0, keepdims=True)
        last = jnp.where(which == 7, 1.0, 0.0)
        bias = seam[...] * last + jnp.where(kept > 0.5, 0.0, NEG)
        diagonal = lax.broadcasted_iota(jnp.int32, (TOK, TOK), 0) == lax.broadcasted_iota(jnp.int32, (TOK, TOK), 1)
        bias = jnp.where(diagonal, 0.0, bias)
        yield
        contexts = []

        def head(scores, vs):
            top = jnp.max(scores, axis=-1, keepdims=True)
            probs = jnp.exp2((scores - top) * LOG2E).astype(BF)
            both = dot(probs, jnp.concatenate([vs, ones], axis=1))
            contexts.append(both[:, :128] * (1.0 / both[:, 128:]))

        waiting = None
        for g in range(2):
            q = (dot(n1, b_qkv[g, 0]).astype(BF)) * BF(HD ** -0.5)
            k = dot(n1, b_qkv[g, 1]).astype(BF)
            val = dot(n1, b_qkv[g, 2]).astype(BF)
            yield
            for pair in range(2):
                cut = slice(128 * pair, 128 * pair + 128)
                for side in range(2):
                    inside = (pair_lane >= 64 * side) & (pair_lane < 64 * side + 64)
                    qs = jnp.where(inside, q[:, cut], BF(0))
                    vs = jnp.where(inside, val[:, cut], BF(0))
                    scores = dot_t(qs, k[:, cut]) + bias
                    if waiting is not None:
                        head(*waiting)
                    waiting = scores, vs
                    yield
        head(*waiting)
        contexts = [(contexts[2 * i] + contexts[2 * i + 1]).astype(BF) for i in range(4)]
        attended = dot(jnp.concatenate(contexts[:2], axis=1), b_proj[0])
        x1 = x + attended + dot(jnp.concatenate(contexts[2:], axis=1), b_proj[1])
        xone[w] = x1
        normed[w] = norm(x1)
        yield

    def finish(w):
        n2 = normed[w]
        for g in range(2):
            for c in range(2):
                h = dot(n2, b_up[g, :, 512 * c : 512 * c + 512])
                h = 0.5 * h * (1.0 + lax.erf(h * (2.0 ** -0.5)))
                hidden[:, 1024 * g + 512 * c : 1024 * g + 512 * c + 512] = h.astype(BF)
                yield
        grown = xone[w] + dot(hidden[:, :1024], b_down[0]) + dot(hidden[:, 1024:], b_down[1])
        yield
        n3 = norm(grown.astype(BF).astype(F32))
        yield
        by_level = dot(level[...], n3).astype(BF)
        base = jnp.zeros((64, 128), F32)
        all_kg = dot_t(b_kg[...].reshape(1024, 512), by_level)
        yield
        for g in range(2):
            kt = all_kg[256 * g : 256 * g + 256].astype(BF)
            both = dot(qbd[g], kt)
            scores = both[:64] + both[64:]
            s0, s1, s2 = scores[:, :128], scores[:, 128:256], scores[:, 256:]
            top = jnp.maximum(jnp.maximum(s0, s1), s2)
            e0, e1, e2 = (jnp.exp2((s - top) * LOG2E) for s in (s0, s1, s2))
            scale = 1.0 / (e0 + e1 + e2)
            dwt[g, 0] = e0 * scale
            dwt[g, 1] = e1 * scale
            vals = all_kg[512 + 256 * g : 768 + 256 * g]
            last_level = vals[:, 256:]
            d0, d1 = vals[:, :128] - last_level, vals[:, 128:256] - last_level
            for h in range(4):
                diff[g, h, 0] = d0[64 * h : 64 * h + 64]
                diff[g, h, 1] = d1[64 * h : 64 * h + 64]
                base = base + last_level[64 * h : 64 * h + 64]
        yield
        for group in ((0, 1, 2, 3), (4, 5, 6, 7), (8, 9, 10, 11, 12)):
            totals = [base] * len(group)
            for g in range(2):
                for h in range(4):
                    for j in range(2):
                        step = diff[g, h, j]
                        totals = [
                            total + dwt[g, j, 16 * h + l : 16 * h + l + 1, :] * step for total, l in zip(totals, group)
                        ]
            for total, l in zip(totals, group):
                zpix[pl.ds(l, 64, stride=16), :] = total
            yield
        packed = jnp.zeros((dests * rows, 256), F32)
        for a in range(4):
            packed = packed + dot_t(outm[a], zpix[256 * a : 256 * a + 256, :].astype(BF))
        for d in range(dests):
            for side in range(2):
                msg[w, side, d] = packed[rows * d : rows * d + rows, 128 * side : 128 * side + 128].astype(BF)
        yield

    def run(*parts, order=""):
        for which in order:
            next(parts[int(which)], None)
        for part in parts:
            for _ in part:
                pass

    my_window = lax.rem(me + grid - dests // 2, grid) // dests

    def send(w):
        base = window_of(v, w) * dests + dests // 2
        stays = window_of(v, w) == my_window

        def one(d, side, to):
            return remote(msg.at[w, side, d], recv.at[me], osend.at[w], orecv, {"grid": to, "var": side})

        for d in range(dests):
            to = (base + d) & (grid - 1)
            one(d, 1 - v, to).start()

            @pl.when(jnp.logical_not(stays & (to == me)))
            def _():
                one(d, v, to).start()

        @pl.when(stays)
        def _():
            d = (me - base) & (grid - 1)
            pltpu.make_async_copy(msg.at[w, v, d], recv.at[me], orecv).start()

    first = lax.rem(me, SLOTS)
    halo(first).wait_recv()
    shared[0].wait()
    shared[1].wait()
    run(attend(first))
    hear(1)
    tell(2)
    for copy in shared[2:]:
        copy.wait()
    lane2 = lax.broadcasted_iota(jnp.int32, (16, 256), 1)
    for g in range(2):
        dq = b_dq[g] * (HD ** -0.5)
        for h in range(4):
            part = jnp.where((lane2 >= 64 * h) & (lane2 < 64 * h + 64), dq, 0.0)
            hi = part.astype(BF)
            qbd[g, 16 * h : 16 * h + 16, :] = hi
            qbd[g, 64 + 16 * h : 80 + 16 * h, :] = (part - hi.astype(F32)).astype(BF)


    def body(step, _):
        now, later = lax.rem(me + step, SLOTS), lax.rem(me + step + 1, SLOTS)
        halo(later).wait_recv()
        run(finish(now), attend(later), order="10000010110101101101101")

        @pl.when(step == 0)
        def _():
            hear(2)
            tell(3)
            hear(3)

        send(now)
        return 0

    lax.fori_loop(0, SLOTS - 1, body, 0)
    last = lax.rem(me + SLOTS - 1, SLOTS)
    run(finish(last))
    send(last)

    def sent(w, _):
        halo(w).wait_send()
        stays = window_of(v, w) == my_window
        row = recv.at[pl.ds(0, 2 * dests)]
        most = recv.at[pl.ds(0, 2 * dests - 1)]

        @pl.when(stays)
        def _():
            pltpu.make_async_copy(most, most, osend.at[w]).wait()

        @pl.when(jnp.logical_not(stays))
        def _():
            pltpu.make_async_copy(row, row, osend.at[w]).wait()

        return 0

    lax.fori_loop(0, SLOTS, sent, 0)
    pltpu.make_async_copy(recv, recv, orecv).wait()


def final_tables(grid):
    _, band, _ = sizes(grid)
    pad = -(-26 * band // 16) * 16
    rows = np.zeros((band, 4 * pad, 128), np.float32)
    for slot in range(band):
        for b in range(4):
            for l in range(NLEV):
                for v in range(2):
                    rows[slot, b * pad + (l * band + slot) * 2 + v, (b * 2 + v) * 16 + l] = 1
    tile = np.gcd(12 * grid, 128)
    spread = np.zeros((4, tile, 4 * tile), np.float32)
    for b in range(4):
        spread[b, np.arange(tile), 4 * np.arange(tile) + b] = 1
    return jnp.asarray(rows, BF), jnp.asarray(spread.reshape(2, 2 * tile, 4 * tile), BF)


def final_kernel(grid, recv, sel, spread, out, stage):
    _, band, _ = sizes(grid)
    cells = 12 * grid
    pad = sel.shape[1] // 4
    for s in range(grid):
        block = recv[s].astype(F32)
        start = 12 * s + 6
        for slot in range(band):
            piece = block[12 * slot : 12 * slot + 12]
            if start + 12 <= cells:
                stage[slot, start : start + 12, :] = piece
            else:
                stage[slot, start : start + 6, :] = piece[:6]
                stage[slot, 0:6, :] = piece[6:]
    flipped = jnp.zeros((4 * pad, cells), F32)
    for slot in range(band):
        flipped = flipped + dot_t(sel[slot], stage[slot].astype(BF))
    flipped = flipped.astype(BF)
    tile = spread.shape[2] // 4
    tiles = cells // tile

    def stacked(b):
        return jnp.concatenate(
            [flipped[b * pad : b * pad + pad, tile * m : tile * m + tile] for m in range(tiles)], axis=0
        )

    lines = dot(jnp.concatenate([stacked(0), stacked(1)], axis=1), spread[0]) + dot(
        jnp.concatenate([stacked(2), stacked(3)], axis=1), spread[1]
    )
    for m in range(tiles):
        for k in range(NLEV * band):
            out[k, :, 4 * tile * m : 4 * tile * (m + 1)] = lines[m * pad + 2 * k : m * pad + 2 * k + 2]


def pixels_of(grid, tokens, key_mask, w_qkv, w_proj, w_up, w_down, level_query, w_dec_q, w_dec_kv, w_dec_o, decode_matrix):
    dests, band, rows = sizes(grid)
    by_column = jnp.transpose(tokens, (1, 2, 0, 3)).reshape(36, 48, 512)
    tables = main_tables(grid)
    operands = (
        by_column, key_mask.T, w_qkv, w_proj, w_up, w_down, level_query, w_dec_q, w_dec_kv, w_dec_o, decode_matrix.T,
    ) + tables
    vm = pltpu.VMEM
    return pl.pallas_call(
        functools.partial(main_kernel, grid),
        out_shape=pltpu.VMEM((grid, rows, 128), BF),
        in_specs=[pl.BlockSpec(memory_space=pltpu.HBM)] * len(operands),
        out_specs=pl.BlockSpec(memory_space=pltpu.VMEM),
        scratch_shapes=[
            vm((36, 48, 512), BF),
            vm((SLOTS, HALF, 512), BF),
            vm((SLOTS, HALF, 512), BF),
            vm((SLOTS, HALF, 512), BF),
            vm((SLOTS, TOK, 512), F32),
            vm((SLOTS, TOK, 512), BF),
            vm((2, 3, 512, 256), BF),
            vm((2, 256, 512), BF),
            vm((2, 512, 1024), BF),
            vm((2, 1024, 512), BF),
            vm((4, 256, 512), BF),
            vm((2, 16, 256), F32),
            vm((2, 128, 256), BF),
            vm((13, 512), BF),
            vm((512, 256), BF),
            vm((2, 512, 256), BF),
            vm((256, 512), BF),
            vm((64, 512), F32),
            *[vm(table.shape[1:] if i < 2 else table.shape, table.dtype) for i, table in enumerate(tables)],
            vm((12, 48), jnp.int32),
            vm((12, 48), jnp.int32),
            vm((32, 48), F32),
            vm((TOK, 2048), BF),
            vm((2, 4, 2, 64, 128), F32),
            vm((2, 2, 64, 128), F32),
            vm((1024, 128), F32),
            vm((SLOTS, 2, dests, rows, 128), BF),
            pltpu.SemaphoreType.DMA((20,)),
            pltpu.SemaphoreType.DMA((7,)),
            pltpu.SemaphoreType.DMA((7,)),
            pltpu.SemaphoreType.DMA((SLOTS + 1,)),
            pltpu.SemaphoreType.DMA((SLOTS + 1,)),
            pltpu.SemaphoreType.DMA((SLOTS,)),
            pltpu.SemaphoreType.DMA,
            pltpu.SemaphoreType.REGULAR((4,)),
        ],
        compiler_params=pltpu.CompilerParams(
            collective_id=0, has_side_effects=True, vmem_limit_bytes=60 * 2**20
        ),
    )(*operands)


def assemble(grid, received):
    _, band, _ = sizes(grid)
    tables = final_tables(grid)
    lines = pl.pallas_call(
        functools.partial(final_kernel, grid),
        in_specs=[pl.BlockSpec(memory_space=pltpu.VMEM)] * 3,
        out_shape=jax.ShapeDtypeStruct((NLEV * band, 2, 48 * grid), F32),
        scratch_shapes=[pltpu.VMEM((band, 12 * grid, 128), F32)],
        compiler_params=pltpu.CompilerParams(vmem_limit_bytes=32 * 2**20),
    )(received, *tables)
    return jnp.transpose(lines.reshape(NLEV, band, 2, 48 * grid), (2, 0, 1, 3))


def local(*args):
    grid = lax.axis_size("grid")
    return assemble(grid, pixels_of(grid, *args))


def solution(mesh):
    placed = (
        P("group", "grid", None, None),
        P("group", "grid"),
        P(None, None, "var"),
        P("var", None),
        P(None, "var"),
        P("var", None),
        P(),
        P(None, "var"),
        P(None, None, "var"),
        P("var", None),
        P(),
    )
    return jax.shard_map(
        local, mesh=mesh, in_specs=placed, out_specs=P("var", "group", "grid", None), check_vma=False
    )
```

```python
import functools

import jax
import jax.numpy as jnp
import numpy as np
from jax import lax
from jax.experimental import pallas as pl
from jax.experimental.pallas import tpu as pltpu
from jax.sharding import PartitionSpec as P

HD = 64
WIN = 6
LEV = 3
PIX = 4
NLEV = 13
HALF = 112
TOK = 2 * HALF
EPSILON = 1e-05
LOG2E = 1.4426950408889634
NEG = -1e30
BF = jnp.bfloat16
F32 = jnp.float32


SLOTS = 4


def window_of(v, slot):
    return (7 * v + 2 * slot) % 8


def sizes(grid):
    dests = grid // 8
    band = WIN * PIX // dests
    rows = -(-(band * 12) // 8) * 8
    return dests, band, rows


def reach(grid):
    stride = int(round(grid**0.5)) if grid > 8 else 2
    radius = 0
    for k in range(grid):
        ways = [abs(b) + min((k - stride * b) % grid, (stride * b - k) % grid) for b in range(-stride, stride + 1)]
        radius = max(radius, min(ways))
    rounds = max(0, (radius - 1).bit_length() - 1)
    assert rounds <= 2
    return stride, rounds


def token_fields():
    t = np.arange(TOK)
    half, q = t // HALF, t % HALF
    valid = q < 108
    cj, r = q // 6, q % 6
    return half, cj // 3, cj % 3, r, valid


def main_tables(grid):
    dests, band, rows = sizes(grid)
    pick = np.zeros((2, SLOTS * 48, 8 * 48), np.float32)
    pick2 = np.zeros((2, SLOTS * 16, 2 * 48), np.float32)
    for v in range(2):
        for step in range(SLOTS):
            for r in range(6):
                row = (6 * int(window_of(v, step)) + 3 + r) % 48
                for cj in range(8):
                    pick[v, step * 48 + cj * 6 + r, cj * 48 + row] = 1
                for cj in range(2):
                    pick2[v, step * 16 + cj * 6 + r, cj * 48 + row] = 1
    half, c6, j, r, valid = token_fields()
    level_rows = np.zeros((384, TOK), np.float32)
    t = np.arange(TOK)[valid]
    patch = half * 36 + c6 * 6 + r
    level_rows[j[valid] * 128 + patch[valid], t] = 1
    out_rows = np.zeros((4, dests * rows, 128), np.float32)
    for d in range(dests):
        for slot in range(band):
            rr, a = divmod(band * d + slot, 4)
            for c in range(12):
                out_rows[a, d * rows + slot * 12 + c, (c // 6) * 36 + (c % 6) * 6 + rr] = 1
    mask_rows = np.zeros((8, 48, TOK), np.float32)
    for window in range(8):
        mask_rows[window, ((6 * window + 3 + r) % 48)[valid], t] = 1
    mask_cols = np.zeros((32, TOK), np.float32)
    mask_cols[np.where(half == 0, 6 + c6, 16 + c6)[valid], t] = 1
    seam = np.where((r >= 3)[:, None] == (r >= 3)[None, :], 0, NEG).astype(np.float32)
    order = np.zeros((64, 64), np.float32)
    for a in range(4):
        for vh in range(2):
            for b in range(4):
                for v in range(2):
                    order[((a * 2 + vh) * 4 + b) * 2 + v, ((vh * 2 + v) * 4 + a) * 4 + b] = 1
    return (
        jnp.asarray(pick, BF),
        jnp.asarray(pick2, BF),
        jnp.asarray(level_rows, BF),
        jnp.asarray(out_rows, BF),
        jnp.asarray(mask_rows, BF),
        jnp.asarray(mask_cols, F32),
        jnp.asarray(seam, F32),
        jnp.asarray(order, BF),
    )


def dot(a, b):
    return lax.dot_general(a, b, (((1,), (0,)), ((), ())), preferred_element_type=F32)


def dot_t(a, b):
    return lax.dot_general(a, b, (((1,), (1,)), ((), ())), preferred_element_type=F32)


def norm(values):
    center = values - jnp.mean(values, axis=-1, keepdims=True)
    spread = jnp.mean(center * center, axis=-1, keepdims=True)
    return (center * lax.rsqrt(spread + EPSILON)).astype(BF)


def split3(values):
    hi = values.astype(BF)
    rest = values - hi.astype(F32)
    mid = rest.astype(BF)
    return hi, mid, (rest - mid.astype(F32)).astype(BF)


def main_kernel(
    grid,
    tokens, mask, w_qkv, w_proj, w_up, w_down, query, w_dec_q, w_dec_kv, w_dec_o, decode_t,
    c_pick, c_pick2, c_level, c_out, c_mrow, c_mcol, c_seam, c_order,
    recv,
    tok, own, hsend, hrecv, xone, normed, b_qkv, b_proj, b_up, b_down, b_kg, b_dq, qbd,
    v_query, v_dq, v_dkv, v_do, v_dec, pick, pick2, level, outm, mrow, mcol, seam, order,
    mask_own, mask_right, marks, hidden, diff, dwt, zpix, msg,
    lsem, wsend, wrecv, hssem, hrsem, osend, orecv, heard,
):
    dests, band, rows = sizes(grid)
    assert grid & (grid - 1) == 0
    me = lax.axis_index("grid")
    v = lax.axis_index("var")
    partner = {"var": 1 - v}
    west = {"grid": lax.rem(me + grid - 1, grid)}

    barrier = pltpu.get_barrier_semaphore()

    def signal(sem, where):
        pl.semaphore_signal(sem, inc=1, device_id=where, device_id_type=pl.DeviceIdType.MESH)

    stride, rounds = reach(grid)
    sides = (1, grid - 1, stride, grid - stride)
    signal(barrier, partner)
    near = sides + tuple(
        (a + b) % grid for a, b in ((2, 0), (-2, 0), (0, 2 * stride), (0, -2 * stride)) + tuple((x, y * stride) for x in (1, -1) for y in (1, -1))
    )
    for by in near:
        signal(barrier, {"grid": lax.rem(me + by, grid)})

    def tell(k):
        if k < rounds:
            for by in sides:
                signal(heard.at[k], {"grid": lax.rem(me + by * 2 ** (k + 1), grid)})
        elif k == rounds:
            signal(heard.at[k], partner)

    def hear(k):
        if k <= rounds:
            pl.semaphore_wait(heard.at[k], 4 if k < rounds else 1)

    loads = [
        (tokens.at[pl.ds(0, 18)], tok.at[pl.ds(0, 18)]),
        (c_pick.at[v], pick),
        (c_pick2.at[v], pick2),
        (tokens.at[pl.ds(18, 18)], tok.at[pl.ds(18, 18)]),
        (w_dec_o, v_do),
        (decode_t, v_dec),
        (c_order, order),
        (w_dec_kv, v_dkv),
        (query, v_query),
        (w_dec_q, v_dq),
        (mask, mask_own),
        (w_qkv, b_qkv.at[v]),
        (c_mrow, mrow),
        (c_mcol, mcol),
        (c_seam, seam),
        (w_proj, b_proj.at[v]),
        (w_up, b_up.at[v]),
        (w_down, b_down.at[v]),
        (c_level, level),
        (c_out, outm),
    ]
    local = [pltpu.make_async_copy(src, dst, lsem.at[i]) for i, (src, dst) in enumerate(loads)]
    for copy in local:
        copy.start()

    def remote(src, dst, send, recv_sem, where):
        return pltpu.make_async_remote_copy(
            src_ref=src, dst_ref=dst, send_sem=send, recv_sem=recv_sem, device_id=where, device_id_type=pl.DeviceIdType.MESH
        )

    def halo(w):
        return remote(hsend.at[w], hrecv.at[w], hssem.at[w], hrsem.at[w], west)

    weights = [
        (w_qkv, b_qkv.at[v]),
        (w_proj, b_proj.at[v]),
        (w_up, b_up.at[v]),
        (w_down, b_down.at[v]),
        (b_kg.at[v], b_kg.at[v]),
        (b_kg.at[2 + v], b_kg.at[2 + v]),
        (b_dq.at[v], b_dq.at[v]),
    ]
    shared = [remote(src, dst, wsend.at[i], wrecv.at[i], partner) for i, (src, dst) in enumerate(weights)]
    mask_copy = remote(mask, mask_right, hssem.at[SLOTS], hrsem.at[SLOTS], west)

    def pack(part, target):
        for block in range(2):
            src = tok[part + 8 * block : part + 8 * block + 8].reshape(384, 512)
            packed = dot(pick[...], src).astype(BF)
            for w in range(SLOTS):
                target[w, 48 * block : 48 * block + 48, :] = packed[48 * w : 48 * w + 48]
        src = tok[part + 16 : part + 18].reshape(96, 512)
        packed = dot(pick2[...], src).astype(BF)
        for w in range(SLOTS):
            target[w, 96:112, :] = packed[16 * w : 16 * w + 16]

    def send_halo(step):
        halo(lax.rem(me + grid - 1 + step, SLOTS)).start()

    for i in range(3):
        local[i].wait()
    pack(0, hsend)
    pl.semaphore_wait(barrier, 1 + len(near))
    tell(0)
    mask_copy.start()
    send_halo(0)
    shared[0].start()
    shared[1].start()
    send_halo(1)
    shared[2].start()
    send_halo(2)
    shared[3].start()
    send_halo(3)
    local[3].wait()
    pack(18, own)

    for i in range(4, 10):
        local[i].wait()
    dec = v_dec[...]
    hi, mid, low = split3(dec)
    do = v_do[...]
    unembed = (dot_t(hi, do) + dot_t(mid, do) + dot_t(low, do)).astype(BF)
    unembed = dot(order[...], unembed).astype(BF)
    lane = lax.broadcasted_iota(jnp.int32, (64, 256), 1)
    for h in range(4):
        block = jnp.where((lane >= 64 * h) & (lane < 64 * h + 64), unembed.astype(F32), 0).astype(BF)
        b_kg[2 + v, 64 * h : 64 * h + 64, :] = dot_t(block, v_dkv[1]).astype(BF)
    eye = jnp.where(
        lax.broadcasted_iota(jnp.int32, (256, 256), 0) == lax.broadcasted_iota(jnp.int32, (256, 256), 1), 1.0, 0.0
    ).astype(BF)
    b_kg[v] = dot_t(eye, v_dkv[0]).astype(BF)
    b_dq[v, 0:13, :] = dot(v_query[...], v_dq[...])
    b_dq[v, 13:16, :] = jnp.zeros((3, 256), F32)

    for copy in shared[4:]:
        copy.start()
    hear(0)
    tell(1)
    zpix[...] = jnp.zeros_like(zpix)
    marks[...] = jnp.zeros_like(marks)

    for i in range(10, len(local)):
        local[i].wait()
    mask_copy.wait()
    marks[0:12, :] = mask_own[...].astype(F32)
    marks[16:28, :] = mask_right[...].astype(F32)
    pair_lane = lax.broadcasted_iota(jnp.int32, (TOK, 128), 1)
    ones = jnp.ones((TOK, 128), BF)

    def attend(w):
        which = window_of(v, w)
        x = jnp.concatenate([own[w], hrecv[w]], axis=0).astype(F32)
        n1 = norm(x)
        kept = jnp.sum(dot(marks[...].astype(BF), mrow[which]) * mcol[...], axis=0, keepdims=True)
        last = jnp.where(which == 7, 1.0, 0.0)
        bias = seam[...] * last + jnp.where(kept > 0.5, 0.0, NEG)
        diagonal = lax.broadcasted_iota(jnp.int32, (TOK, TOK), 0) == lax.broadcasted_iota(jnp.int32, (TOK, TOK), 1)
        bias = jnp.where(diagonal, 0.0, bias)
        yield
        contexts = []

        def head(scores, vs):
            top = jnp.max(scores, axis=-1, keepdims=True)
            probs = jnp.exp2((scores - top) * LOG2E).astype(BF)
            both = dot(probs, jnp.concatenate([vs, ones], axis=1))
            contexts.append(both[:, :128] * (1.0 / both[:, 128:]))

        waiting = None
        for g in range(2):
            q = (dot(n1, b_qkv[g, 0]).astype(BF)) * BF(HD ** -0.5)
            k = dot(n1, b_qkv[g, 1]).astype(BF)
            val = dot(n1, b_qkv[g, 2]).astype(BF)
            yield
            for pair in range(2):
                cut = slice(128 * pair, 128 * pair + 128)
                for side in range(2):
                    inside = (pair_lane >= 64 * side) & (pair_lane < 64 * side + 64)
                    qs = jnp.where(inside, q[:, cut], BF(0))
                    vs = jnp.where(inside, val[:, cut], BF(0))
                    scores = dot_t(qs, k[:, cut]) + bias
                    if waiting is not None:
                        head(*waiting)
                    waiting = scores, vs
                    yield
        head(*waiting)
        contexts = [(contexts[2 * i] + contexts[2 * i + 1]).astype(BF) for i in range(4)]
        attended = dot(jnp.concatenate(contexts[:2], axis=1), b_proj[0])
        x1 = x + attended + dot(jnp.concatenate(contexts[2:], axis=1), b_proj[1])
        xone[w] = x1
        normed[w] = norm(x1)
        yield

    def finish(w):
        n2 = normed[w]
        for g in range(2):
            for c in range(2):
                h = dot(n2, b_up[g, :, 512 * c : 512 * c + 512])
                h = h * (1.0 + lax.erf(h * (2.0 ** -0.5)))
                hidden[:, 1024 * g + 512 * c : 1024 * g + 512 * c + 512] = h.astype(BF)
                yield
        grown = xone[w] + 0.5 * (dot(hidden[:, :1024], b_down[0]) + dot(hidden[:, 1024:], b_down[1]))
        yield
        n3 = norm(grown.astype(BF).astype(F32))
        yield
        by_level = dot(level[...], n3).astype(BF)
        base = jnp.zeros((64, 128), F32)
        all_kg = dot_t(b_kg[...].reshape(1024, 512), by_level)
        yield
        for g in range(2):
            kt = all_kg[256 * g : 256 * g + 256].astype(BF)
            both = dot(qbd[g], kt)
            scores = both[:64] + both[64:]
            s0, s1, s2 = scores[:, :128], scores[:, 128:256], scores[:, 256:]
            top = jnp.maximum(jnp.maximum(s0, s1), s2)
            e0, e1, e2 = (jnp.exp2((s - top) * LOG2E) for s in (s0, s1, s2))
            scale = 1.0 / (e0 + e1 + e2)
            dwt[g, 0] = e0 * scale
            dwt[g, 1] = e1 * scale
            vals = all_kg[512 + 256 * g : 768 + 256 * g]
            last_level = vals[:, 256:]
            d0, d1 = vals[:, :128] - last_level, vals[:, 128:256] - last_level
            for h in range(4):
                diff[g, h, 0] = d0[64 * h : 64 * h + 64]
                diff[g, h, 1] = d1[64 * h : 64 * h + 64]
                base = base + last_level[64 * h : 64 * h + 64]
        yield
        for group in ((0, 1, 2, 3), (4, 5, 6, 7), (8, 9, 10, 11, 12)):
            totals = [base] * len(group)
            for g in range(2):
                for h in range(4):
                    for j in range(2):
                        step = diff[g, h, j]
                        totals = [
                            total + dwt[g, j, 16 * h + l : 16 * h + l + 1, :] * step for total, l in zip(totals, group)
                        ]
            for total, l in zip(totals, group):
                zpix[pl.ds(l, 64, stride=16), :] = total
            yield
        packed = jnp.zeros((dests * rows, 256), F32)
        for a in range(4):
            packed = packed + dot_t(outm[a], zpix[256 * a : 256 * a + 256, :].astype(BF))
        for d in range(dests):
            for side in range(2):
                msg[w, side, d] = packed[rows * d : rows * d + rows, 128 * side : 128 * side + 128].astype(BF)
        yield

    def run(*parts, order=""):
        for which in order:
            next(parts[int(which)], None)
        for part in parts:
            for _ in part:
                pass

    my_window = lax.rem(me + grid - dests // 2, grid) // dests

    def send(w):
        base = window_of(v, w) * dests + dests // 2
        stays = window_of(v, w) == my_window

        def one(d, side, to):
            return remote(msg.at[w, side, d], recv.at[me], osend.at[w], orecv, {"grid": to, "var": side})

        @pl.when(jnp.logical_not(stays))
        def _():
            for d in range(dests):
                for side in range(2):
                    one(d, side, (base + d) & (grid - 1)).start()

        @pl.when(stays)
        def _():
            own_band = (me - base) & (grid - 1)

            def away(k, _):
                d = (own_band + k) & (dests - 1)
                for side in range(2):
                    one(d, side, (base + d) & (grid - 1)).start()
                return 0

            lax.fori_loop(1, dests, away, 0)
            one(own_band, 1 - v, me).start()
            pltpu.make_async_copy(msg.at[w, v, own_band], recv.at[me], orecv).start()

    first = lax.rem(me, SLOTS)
    halo(first).wait_recv()
    shared[0].wait()
    shared[1].wait()
    run(attend(first))
    hear(1)
    tell(2)
    for copy in shared[2:]:
        copy.wait()
    lane2 = lax.broadcasted_iota(jnp.int32, (16, 256), 1)
    for g in range(2):
        dq = b_dq[g] * (HD ** -0.5)
        for h in range(4):
            part = jnp.where((lane2 >= 64 * h) & (lane2 < 64 * h + 64), dq, 0.0)
            hi = part.astype(BF)
            qbd[g, 16 * h : 16 * h + 16, :] = hi
            qbd[g, 64 + 16 * h : 80 + 16 * h, :] = (part - hi.astype(F32)).astype(BF)


    def body(step, _):
        now, later = lax.rem(me + step, SLOTS), lax.rem(me + step + 1, SLOTS)
        halo(later).wait_recv()
        run(finish(now), attend(later), order="10000010110101101101101")

        @pl.when(step == 0)
        def _():
            hear(2)
            tell(3)
            hear(3)

        send(now)
        return 0

    lax.fori_loop(0, SLOTS - 1, body, 0)
    last = lax.rem(me + SLOTS - 1, SLOTS)
    run(finish(last))
    send(last)

    def sent(w, _):
        halo(w).wait_send()
        stays = window_of(v, w) == my_window
        row = recv.at[pl.ds(0, 2 * dests)]
        most = recv.at[pl.ds(0, 2 * dests - 1)]

        @pl.when(stays)
        def _():
            pltpu.make_async_copy(most, most, osend.at[w]).wait()

        @pl.when(jnp.logical_not(stays))
        def _():
            pltpu.make_async_copy(row, row, osend.at[w]).wait()

        return 0

    lax.fori_loop(0, SLOTS, sent, 0)
    pltpu.make_async_copy(recv, recv, orecv).wait()


def final_tables(grid):
    _, band, _ = sizes(grid)
    pad = -(-26 * band // 16) * 16
    rows = np.zeros((band, 4 * pad, 128), np.float32)
    for slot in range(band):
        for b in range(4):
            for l in range(NLEV):
                for v in range(2):
                    rows[slot, b * pad + (l * band + slot) * 2 + v, (b * 2 + v) * 16 + l] = 1
    tile = np.gcd(12 * grid, 128)
    spread = np.zeros((4, tile, 4 * tile), np.float32)
    for b in range(4):
        spread[b, np.arange(tile), 4 * np.arange(tile) + b] = 1
    return jnp.asarray(rows, BF), jnp.asarray(spread.reshape(2, 2 * tile, 4 * tile), BF)


def final_kernel(grid, recv, sel, spread, out, stage):
    _, band, _ = sizes(grid)
    cells = 12 * grid
    pad = sel.shape[1] // 4
    for s in range(grid):
        block = recv[s].astype(F32)
        start = 12 * s + 6
        for slot in range(band):
            piece = block[12 * slot : 12 * slot + 12]
            if start + 12 <= cells:
                stage[slot, start : start + 12, :] = piece
            else:
                stage[slot, start : start + 6, :] = piece[:6]
                stage[slot, 0:6, :] = piece[6:]
    flipped = jnp.zeros((4 * pad, cells), F32)
    for slot in range(0, band, 2):
        group = range(slot, min(slot + 2, band))
        picks = jnp.concatenate([sel[k] for k in group], axis=1)
        cells_of = jnp.concatenate([stage[k].astype(BF) for k in group], axis=1)
        flipped = flipped + dot_t(picks, cells_of)
    flipped = flipped.astype(BF)
    tile = spread.shape[2] // 4
    tiles = cells // tile

    def stacked(b):
        return jnp.concatenate(
            [flipped[b * pad : b * pad + pad, tile * m : tile * m + tile] for m in range(tiles)], axis=0
        )

    lines = dot(jnp.concatenate([stacked(0), stacked(1)], axis=1), spread[0]) + dot(
        jnp.concatenate([stacked(2), stacked(3)], axis=1), spread[1]
    )
    for m in range(tiles):
        for k in range(NLEV * band):
            out[k, :, 4 * tile * m : 4 * tile * (m + 1)] = lines[m * pad + 2 * k : m * pad + 2 * k + 2]


def pixels_of(grid, tokens, key_mask, w_qkv, w_proj, w_up, w_down, level_query, w_dec_q, w_dec_kv, w_dec_o, decode_matrix):
    dests, band, rows = sizes(grid)
    by_column = jnp.transpose(tokens, (1, 2, 0, 3)).reshape(36, 48, 512)
    tables = main_tables(grid)
    operands = (
        by_column, key_mask.T, w_qkv, w_proj, w_up, w_down, level_query, w_dec_q, w_dec_kv, w_dec_o, decode_matrix.T,
    ) + tables
    vm = pltpu.VMEM
    return pl.pallas_call(
        functools.partial(main_kernel, grid),
        out_shape=pltpu.VMEM((grid, rows, 128), BF),
        in_specs=[pl.BlockSpec(memory_space=pltpu.HBM)] * len(operands),
        out_specs=pl.BlockSpec(memory_space=pltpu.VMEM),
        scratch_shapes=[
            vm((36, 48, 512), BF),
            vm((SLOTS, HALF, 512), BF),
            vm((SLOTS, HALF, 512), BF),
            vm((SLOTS, HALF, 512), BF),
            vm((SLOTS, TOK, 512), F32),
            vm((SLOTS, TOK, 512), BF),
            vm((2, 3, 512, 256), BF),
            vm((2, 256, 512), BF),
            vm((2, 512, 1024), BF),
            vm((2, 1024, 512), BF),
            vm((4, 256, 512), BF),
            vm((2, 16, 256), F32),
            vm((2, 128, 256), BF),
            vm((13, 512), BF),
            vm((512, 256), BF),
            vm((2, 512, 256), BF),
            vm((256, 512), BF),
            vm((64, 512), F32),
            *[vm(table.shape[1:] if i < 2 else table.shape, table.dtype) for i, table in enumerate(tables)],
            vm((12, 48), jnp.int32),
            vm((12, 48), jnp.int32),
            vm((32, 48), F32),
            vm((TOK, 2048), BF),
            vm((2, 4, 2, 64, 128), F32),
            vm((2, 2, 64, 128), F32),
            vm((1024, 128), F32),
            vm((SLOTS, 2, dests, rows, 128), BF),
            pltpu.SemaphoreType.DMA((20,)),
            pltpu.SemaphoreType.DMA((7,)),
            pltpu.SemaphoreType.DMA((7,)),
            pltpu.SemaphoreType.DMA((SLOTS + 1,)),
            pltpu.SemaphoreType.DMA((SLOTS + 1,)),
            pltpu.SemaphoreType.DMA((SLOTS,)),
            pltpu.SemaphoreType.DMA,
            pltpu.SemaphoreType.REGULAR((4,)),
        ],
        compiler_params=pltpu.CompilerParams(
            collective_id=0, has_side_effects=True, vmem_limit_bytes=60 * 2**20
        ),
    )(*operands)


def assemble(grid, received):
    _, band, _ = sizes(grid)
    tables = final_tables(grid)
    lines = pl.pallas_call(
        functools.partial(final_kernel, grid),
        in_specs=[pl.BlockSpec(memory_space=pltpu.VMEM)] * 3,
        out_shape=jax.ShapeDtypeStruct((NLEV * band, 2, 48 * grid), F32),
        scratch_shapes=[pltpu.VMEM((band, 12 * grid, 128), F32)],
        compiler_params=pltpu.CompilerParams(vmem_limit_bytes=32 * 2**20),
    )(received, *tables)
    return jnp.transpose(lines.reshape(NLEV, band, 2, 48 * grid), (2, 0, 1, 3))


def local(*args):
    grid = lax.axis_size("grid")
    return assemble(grid, pixels_of(grid, *args))


def solution(mesh):
    placed = (
        P("group", "grid", None, None),
        P("group", "grid"),
        P(None, None, "var"),
        P("var", None),
        P(None, "var"),
        P("var", None),
        P(),
        P(None, "var"),
        P(None, None, "var"),
        P("var", None),
        P(),
    )
    return jax.shard_map(
        local, mesh=mesh, in_specs=placed, out_specs=P("var", "group", "grid", None), check_vma=False
    )
```

```python
import functools

import jax
import jax.numpy as jnp
import numpy as np
from jax import lax
from jax.experimental import pallas as pl
from jax.experimental.pallas import tpu as pltpu
from jax.sharding import PartitionSpec as P

HD = 64
WIN = 6
LEV = 3
PIX = 4
NLEV = 13
HALF = 112
TOK = 2 * HALF
EPSILON = 1e-05
LOG2E = 1.4426950408889634
NEG = -1e30
BF = jnp.bfloat16
F32 = jnp.float32


SLOTS = 4


def window_of(v, slot):
    return (7 * v + 2 * slot) % 8


def sizes(grid):
    dests = grid // 8
    band = WIN * PIX // dests
    return dests, band, band * 12


def pitch_of(rows):
    return -(-rows // 8) * 8


def reach(grid):
    stride = int(round(grid**0.5)) if grid > 8 else 2
    radius = 0
    for k in range(grid):
        ways = [abs(b) + min((k - stride * b) % grid, (stride * b - k) % grid) for b in range(-stride, stride + 1)]
        radius = max(radius, min(ways))
    rounds = max(0, (radius - 1).bit_length() - 1)
    assert rounds <= 2
    return stride, rounds


def token_fields():
    t = np.arange(TOK)
    half, q = t // HALF, t % HALF
    valid = q < 108
    cj, r = q // 6, q % 6
    return half, cj // 3, cj % 3, r, valid


def main_tables(grid):
    dests, band, rows = sizes(grid)
    pick = np.zeros((2, SLOTS * 48, 8 * 48), np.float32)
    pick2 = np.zeros((2, SLOTS * 16, 2 * 48), np.float32)
    for v in range(2):
        for step in range(SLOTS):
            for r in range(6):
                row = (6 * int(window_of(v, step)) + 3 + r) % 48
                for cj in range(8):
                    pick[v, step * 48 + cj * 6 + r, cj * 48 + row] = 1
                for cj in range(2):
                    pick2[v, step * 16 + cj * 6 + r, cj * 48 + row] = 1
    half, c6, j, r, valid = token_fields()
    level_rows = np.zeros((384, TOK), np.float32)
    t = np.arange(TOK)[valid]
    patch = half * 36 + c6 * 6 + r
    level_rows[j[valid] * 128 + patch[valid], t] = 1
    pitch = pitch_of(rows)
    out_rows = np.zeros((4, dests * pitch, 128), np.float32)
    for d in range(dests):
        for slot in range(band):
            rr, a = divmod(band * d + slot, 4)
            for c in range(12):
                out_rows[a, d * pitch + slot * 12 + c, (c // 6) * 36 + (c % 6) * 6 + rr] = 1
    mask_rows = np.zeros((8, 48, TOK), np.float32)
    for window in range(8):
        mask_rows[window, ((6 * window + 3 + r) % 48)[valid], t] = 1
    mask_cols = np.zeros((32, TOK), np.float32)
    mask_cols[np.where(half == 0, 6 + c6, 16 + c6)[valid], t] = 1
    seam = np.where((r >= 3)[:, None] == (r >= 3)[None, :], 0, NEG).astype(np.float32)
    order = np.zeros((64, 64), np.float32)
    for a in range(4):
        for vh in range(2):
            for b in range(4):
                for v in range(2):
                    order[((a * 2 + vh) * 4 + b) * 2 + v, ((vh * 2 + v) * 4 + a) * 4 + b] = 1
    return (
        jnp.asarray(pick, BF),
        jnp.asarray(pick2, BF),
        jnp.asarray(level_rows, BF),
        jnp.asarray(out_rows, BF),
        jnp.asarray(mask_rows, BF),
        jnp.asarray(mask_cols, F32),
        jnp.asarray(seam, F32),
        jnp.asarray(order, BF),
    )


def dot(a, b):
    return lax.dot_general(a, b, (((1,), (0,)), ((), ())), preferred_element_type=F32)


def dot_t(a, b):
    return lax.dot_general(a, b, (((1,), (1,)), ((), ())), preferred_element_type=F32)


def norm(values):
    center = values - jnp.mean(values, axis=-1, keepdims=True)
    spread = jnp.mean(center * center, axis=-1, keepdims=True)
    return (center * lax.rsqrt(spread + EPSILON)).astype(BF)


def split3(values):
    hi = values.astype(BF)
    rest = values - hi.astype(F32)
    mid = rest.astype(BF)
    return hi, mid, (rest - mid.astype(F32)).astype(BF)


def main_kernel(
    grid,
    tokens, mask, w_qkv, w_proj, w_up, w_down, query, w_dec_q, w_dec_kv, w_dec_o, decode_t,
    c_pick, c_pick2, c_level, c_out, c_mrow, c_mcol, c_seam, c_order,
    recv,
    tok, own, hsend, hrecv, xone, normed, b_qkv, b_proj, b_up, b_down, b_kg, b_dq, qbd,
    v_query, v_dq, v_dkv, v_do, v_dec, pick, pick2, level, outm, mrow, mcol, seam, order,
    mask_own, mask_right, marks, hidden, diff, dwt, zpix, msg,
    lsem, wsend, wrecv, hssem, hrsem, osend, orecv, heard,
):
    dests, band, rows = sizes(grid)
    assert grid & (grid - 1) == 0
    me = lax.axis_index("grid")
    v = lax.axis_index("var")
    partner = {"var": 1 - v}
    west = {"grid": lax.rem(me + grid - 1, grid)}

    barrier = pltpu.get_barrier_semaphore()

    def signal(sem, where):
        pl.semaphore_signal(sem, inc=1, device_id=where, device_id_type=pl.DeviceIdType.MESH)

    stride, rounds = reach(grid)
    sides = (1, grid - 1, stride, grid - stride)
    signal(barrier, partner)
    near = sides + tuple(
        (a + b) % grid for a, b in ((2, 0), (-2, 0), (0, 2 * stride), (0, -2 * stride)) + tuple((x, y * stride) for x in (1, -1) for y in (1, -1))
    )
    for by in near:
        signal(barrier, {"grid": lax.rem(me + by, grid)})

    def tell(k):
        if k < rounds:
            for by in sides:
                signal(heard.at[k], {"grid": lax.rem(me + by * 2 ** (k + 1), grid)})
        elif k == rounds:
            signal(heard.at[k], partner)

    def hear(k):
        if k <= rounds:
            pl.semaphore_wait(heard.at[k], 4 if k < rounds else 1)

    loads = [
        (tokens.at[pl.ds(0, 18)], tok.at[pl.ds(0, 18)]),
        (c_pick.at[v], pick),
        (c_pick2.at[v], pick2),
        (tokens.at[pl.ds(18, 18)], tok.at[pl.ds(18, 18)]),
        (w_dec_o, v_do),
        (decode_t, v_dec),
        (c_order, order),
        (w_dec_kv, v_dkv),
        (query, v_query),
        (w_dec_q, v_dq),
        (mask, mask_own),
        (w_qkv, b_qkv.at[v]),
        (c_mrow, mrow),
        (c_mcol, mcol),
        (c_seam, seam),
        (w_proj, b_proj.at[v]),
        (w_up, b_up.at[v]),
        (w_down, b_down.at[v]),
        (c_level, level),
        (c_out, outm),
    ]
    local = [pltpu.make_async_copy(src, dst, lsem.at[i]) for i, (src, dst) in enumerate(loads)]
    for copy in local:
        copy.start()

    def remote(src, dst, send, recv_sem, where):
        return pltpu.make_async_remote_copy(
            src_ref=src, dst_ref=dst, send_sem=send, recv_sem=recv_sem, device_id=where, device_id_type=pl.DeviceIdType.MESH
        )

    def halo(w):
        return remote(hsend.at[w], hrecv.at[w], hssem.at[w], hrsem.at[w], west)

    weights = [
        (w_qkv, b_qkv.at[v]),
        (w_proj, b_proj.at[v]),
        (w_up, b_up.at[v]),
        (w_down, b_down.at[v]),
        (b_kg.at[v], b_kg.at[v]),
        (b_kg.at[2 + v], b_kg.at[2 + v]),
        (b_dq.at[v], b_dq.at[v]),
    ]
    shared = [remote(src, dst, wsend.at[i], wrecv.at[i], partner) for i, (src, dst) in enumerate(weights)]
    mask_copy = remote(mask, mask_right, hssem.at[SLOTS], hrsem.at[SLOTS], west)

    def pack(part, target):
        for block in range(2):
            src = tok[part + 8 * block : part + 8 * block + 8].reshape(384, 512)
            packed = dot(pick[...], src).astype(BF)
            for w in range(SLOTS):
                target[w, 48 * block : 48 * block + 48, :] = packed[48 * w : 48 * w + 48]
        src = tok[part + 16 : part + 18].reshape(96, 512)
        packed = dot(pick2[...], src).astype(BF)
        for w in range(SLOTS):
            target[w, 96:112, :] = packed[16 * w : 16 * w + 16]

    def send_halo(step):
        halo(lax.rem(me + grid - 1 + step, SLOTS)).start()

    for i in range(3):
        local[i].wait()
    pack(0, hsend)
    pl.semaphore_wait(barrier, 1 + len(near))
    tell(0)
    send_halo(0)
    mask_copy.start()
    shared[0].start()
    shared[1].start()
    send_halo(1)
    shared[2].start()
    send_halo(2)
    shared[3].start()
    send_halo(3)
    local[3].wait()
    pack(18, own)

    for i in range(4, 10):
        local[i].wait()
    dec = v_dec[...]
    hi, mid, low = split3(dec)
    do = v_do[...]
    unembed = (dot_t(hi, do) + dot_t(mid, do) + dot_t(low, do)).astype(BF)
    unembed = dot(order[...], unembed).astype(BF)
    lane = lax.broadcasted_iota(jnp.int32, (64, 256), 1)
    for h in range(4):
        block = jnp.where((lane >= 64 * h) & (lane < 64 * h + 64), unembed.astype(F32), 0).astype(BF)
        b_kg[2 + v, 64 * h : 64 * h + 64, :] = dot_t(block, v_dkv[1]).astype(BF)
    eye = jnp.where(
        lax.broadcasted_iota(jnp.int32, (256, 256), 0) == lax.broadcasted_iota(jnp.int32, (256, 256), 1), 1.0, 0.0
    ).astype(BF)
    b_kg[v] = dot_t(eye, v_dkv[0]).astype(BF)
    b_dq[v, 0:13, :] = dot(v_query[...], v_dq[...])
    b_dq[v, 13:16, :] = jnp.zeros((3, 256), F32)

    for copy in shared[4:]:
        copy.start()
    hear(0)
    tell(1)
    zpix[...] = jnp.zeros_like(zpix)
    marks[...] = jnp.zeros_like(marks)

    for i in range(10, len(local)):
        local[i].wait()
    mask_copy.wait()
    marks[0:12, :] = mask_own[...].astype(F32)
    marks[16:28, :] = mask_right[...].astype(F32)
    pair_lane = lax.broadcasted_iota(jnp.int32, (TOK, 128), 1)
    ones = jnp.ones((TOK, 128), BF)

    def attend(w):
        which = window_of(v, w)
        x = jnp.concatenate([own[w], hrecv[w]], axis=0).astype(F32)
        n1 = norm(x)
        kept = jnp.sum(dot(marks[...].astype(BF), mrow[which]) * mcol[...], axis=0, keepdims=True)
        last = jnp.where(which == 7, 1.0, 0.0)
        bias = seam[...] * last + jnp.where(kept > 0.5, 0.0, NEG)
        diagonal = lax.broadcasted_iota(jnp.int32, (TOK, TOK), 0) == lax.broadcasted_iota(jnp.int32, (TOK, TOK), 1)
        bias = jnp.where(diagonal, 0.0, bias)
        yield
        contexts = []

        def head(scores, vs):
            top = jnp.max(scores, axis=-1, keepdims=True)
            probs = jnp.exp2((scores - top) * LOG2E).astype(BF)
            both = dot(probs, jnp.concatenate([vs, ones], axis=1))
            contexts.append(both[:, :128] * (1.0 / both[:, 128:]))

        waiting = None
        for g in range(2):
            q = (dot(n1, b_qkv[g, 0]).astype(BF)) * BF(HD ** -0.5)
            k = dot(n1, b_qkv[g, 1]).astype(BF)
            val = dot(n1, b_qkv[g, 2]).astype(BF)
            yield
            for pair in range(2):
                cut = slice(128 * pair, 128 * pair + 128)
                for side in range(2):
                    inside = (pair_lane >= 64 * side) & (pair_lane < 64 * side + 64)
                    qs = jnp.where(inside, q[:, cut], BF(0))
                    vs = jnp.where(inside, val[:, cut], BF(0))
                    scores = dot_t(qs, k[:, cut]) + bias
                    if waiting is not None:
                        head(*waiting)
                    waiting = scores, vs
                    yield
        head(*waiting)
        contexts = [(contexts[2 * i] + contexts[2 * i + 1]).astype(BF) for i in range(4)]
        attended = dot(jnp.concatenate(contexts[:2], axis=1), b_proj[0])
        x1 = x + attended + dot(jnp.concatenate(contexts[2:], axis=1), b_proj[1])
        xone[w] = x1
        normed[w] = norm(x1)
        yield

    def finish(w):
        n2 = normed[w]
        for g in range(2):
            for c in range(2):
                h = dot(n2, b_up[g, :, 512 * c : 512 * c + 512])
                h = h * (1.0 + lax.erf(h * (2.0 ** -0.5)))
                hidden[:, 1024 * g + 512 * c : 1024 * g + 512 * c + 512] = h.astype(BF)
                yield
        grown = xone[w] + 0.5 * (dot(hidden[:, :1024], b_down[0]) + dot(hidden[:, 1024:], b_down[1]))
        yield
        n3 = norm(grown.astype(BF).astype(F32))
        yield
        by_level = dot(level[...], n3).astype(BF)
        base = jnp.zeros((64, 128), F32)
        all_kg = dot_t(b_kg[...].reshape(1024, 512), by_level)
        yield
        for g in range(2):
            kt = all_kg[256 * g : 256 * g + 256].astype(BF)
            both = dot(qbd[g], kt)
            scores = both[:64] + both[64:]
            s0, s1, s2 = scores[:, :128], scores[:, 128:256], scores[:, 256:]
            top = jnp.maximum(jnp.maximum(s0, s1), s2)
            e0, e1, e2 = (jnp.exp2((s - top) * LOG2E) for s in (s0, s1, s2))
            scale = 1.0 / (e0 + e1 + e2)
            dwt[g, 0] = e0 * scale
            dwt[g, 1] = e1 * scale
            vals = all_kg[512 + 256 * g : 768 + 256 * g]
            last_level = vals[:, 256:]
            d0, d1 = vals[:, :128] - last_level, vals[:, 128:256] - last_level
            for h in range(4):
                diff[g, h, 0] = d0[64 * h : 64 * h + 64]
                diff[g, h, 1] = d1[64 * h : 64 * h + 64]
                base = base + last_level[64 * h : 64 * h + 64]
        yield
        for group in ((0, 1, 2, 3), (4, 5, 6, 7), (8, 9, 10, 11, 12)):
            totals = [base] * len(group)
            for g in range(2):
                for h in range(4):
                    for j in range(2):
                        step = diff[g, h, j]
                        totals = [
                            total + dwt[g, j, 16 * h + l : 16 * h + l + 1, :] * step for total, l in zip(totals, group)
                        ]
            for total, l in zip(totals, group):
                zpix[pl.ds(l, 64, stride=16), :] = total
            yield
        pitch = pitch_of(rows)
        packed = jnp.zeros((dests * pitch, 256), F32)
        for a in range(4):
            packed = packed + dot_t(outm[a], zpix[256 * a : 256 * a + 256, :].astype(BF))
        for d in range(dests):
            for side in range(2):
                msg[w, side, d] = packed[pitch * d : pitch * d + rows, 128 * side : 128 * side + 128].astype(BF)
        yield

    def run(*parts, order=""):
        for which in order:
            next(parts[int(which)], None)
        for part in parts:
            for _ in part:
                pass

    my_window = lax.rem(me + grid - dests // 2, grid) // dests

    def send(w):
        base = window_of(v, w) * dests + dests // 2
        stays = window_of(v, w) == my_window

        def one(d, side, to):
            return remote(msg.at[w, side, d], recv.at[me], osend.at[w], orecv, {"grid": to, "var": side})

        @pl.when(jnp.logical_not(stays))
        def _():
            for d in range(dests):
                for side in range(2):
                    one(d, side, (base + d) & (grid - 1)).start()

        @pl.when(stays)
        def _():
            own_band = (me - base) & (grid - 1)

            def away(k, _):
                d = (own_band + k) & (dests - 1)
                for side in range(2):
                    one(d, side, (base + d) & (grid - 1)).start()
                return 0

            lax.fori_loop(1, dests, away, 0)
            one(own_band, 1 - v, me).start()
            pltpu.make_async_copy(msg.at[w, v, own_band], recv.at[me], orecv).start()

    first = lax.rem(me, SLOTS)
    halo(first).wait_recv()
    shared[0].wait()
    shared[1].wait()
    run(attend(first))
    hear(1)
    tell(2)
    for copy in shared[2:]:
        copy.wait()
    lane2 = lax.broadcasted_iota(jnp.int32, (16, 256), 1)
    for g in range(2):
        dq = b_dq[g] * (HD ** -0.5)
        for h in range(4):
            part = jnp.where((lane2 >= 64 * h) & (lane2 < 64 * h + 64), dq, 0.0)
            hi = part.astype(BF)
            qbd[g, 16 * h : 16 * h + 16, :] = hi
            qbd[g, 64 + 16 * h : 80 + 16 * h, :] = (part - hi.astype(F32)).astype(BF)


    def body(step, _):
        now, later = lax.rem(me + step, SLOTS), lax.rem(me + step + 1, SLOTS)
        halo(later).wait_recv()
        run(finish(now), attend(later), order="10000010110101101101101")

        @pl.when(step == 0)
        def _():
            hear(2)
            tell(3)
            hear(3)

        send(now)
        return 0

    lax.fori_loop(0, SLOTS - 1, body, 0)
    last = lax.rem(me + SLOTS - 1, SLOTS)
    run(finish(last))
    send(last)

    def sent(w, _):
        halo(w).wait_send()
        stays = window_of(v, w) == my_window
        row = recv.at[pl.ds(0, 2 * dests)]
        most = recv.at[pl.ds(0, 2 * dests - 1)]

        @pl.when(stays)
        def _():
            pltpu.make_async_copy(most, most, osend.at[w]).wait()

        @pl.when(jnp.logical_not(stays))
        def _():
            pltpu.make_async_copy(row, row, osend.at[w]).wait()

        return 0

    lax.fori_loop(0, SLOTS, sent, 0)
    pltpu.make_async_copy(recv, recv, orecv).wait()


def final_tables(grid):
    _, band, _ = sizes(grid)
    pad = -(-26 * band // 16) * 16
    rows = np.zeros((band, 4 * pad, 128), np.float32)
    for slot in range(band):
        for b in range(4):
            for l in range(NLEV):
                for v in range(2):
                    rows[slot, b * pad + (l * band + slot) * 2 + v, (b * 2 + v) * 16 + l] = 1
    tile = np.gcd(12 * grid, 128)
    spread = np.zeros((4, tile, 4 * tile), np.float32)
    for b in range(4):
        spread[b, np.arange(tile), 4 * np.arange(tile) + b] = 1
    return jnp.asarray(rows, BF), jnp.asarray(spread.reshape(2, 2 * tile, 4 * tile), BF)


def final_kernel(grid, recv, sel, spread, out, stage):
    _, band, _ = sizes(grid)
    cells = 12 * grid
    pad = sel.shape[1] // 4
    for s in range(grid):
        block = recv[s].astype(F32)
        start = 12 * s + 6
        for slot in range(band):
            piece = block[12 * slot : 12 * slot + 12]
            if start + 12 <= cells:
                stage[slot, start : start + 12, :] = piece
            else:
                stage[slot, start : start + 6, :] = piece[:6]
                stage[slot, 0:6, :] = piece[6:]
    flipped = jnp.zeros((4 * pad, cells), F32)
    for slot in range(0, band, 2):
        group = range(slot, min(slot + 2, band))
        picks = jnp.concatenate([sel[k] for k in group], axis=1)
        cells_of = jnp.concatenate([stage[k].astype(BF) for k in group], axis=1)
        flipped = flipped + dot_t(picks, cells_of)
    flipped = flipped.astype(BF)
    tile = spread.shape[2] // 4
    tiles = cells // tile

    def stacked(b):
        return jnp.concatenate(
            [flipped[b * pad : b * pad + pad, tile * m : tile * m + tile] for m in range(tiles)], axis=0
        )

    lines = dot(jnp.concatenate([stacked(0), stacked(1)], axis=1), spread[0]) + dot(
        jnp.concatenate([stacked(2), stacked(3)], axis=1), spread[1]
    )
    for m in range(tiles):
        for k in range(NLEV * band):
            out[k, :, 4 * tile * m : 4 * tile * (m + 1)] = lines[m * pad + 2 * k : m * pad + 2 * k + 2]


def pixels_of(grid, tokens, key_mask, w_qkv, w_proj, w_up, w_down, level_query, w_dec_q, w_dec_kv, w_dec_o, decode_matrix):
    dests, band, rows = sizes(grid)
    by_column = jnp.transpose(tokens, (1, 2, 0, 3)).reshape(36, 48, 512)
    tables = main_tables(grid)
    operands = (
        by_column, key_mask.T, w_qkv, w_proj, w_up, w_down, level_query, w_dec_q, w_dec_kv, w_dec_o, decode_matrix.T,
    ) + tables
    vm = pltpu.VMEM
    return pl.pallas_call(
        functools.partial(main_kernel, grid),
        out_shape=pltpu.VMEM((grid, rows, 128), BF),
        in_specs=[pl.BlockSpec(memory_space=pltpu.HBM)] * len(operands),
        out_specs=pl.BlockSpec(memory_space=pltpu.VMEM),
        scratch_shapes=[
            vm((36, 48, 512), BF),
            vm((SLOTS, HALF, 512), BF),
            vm((SLOTS, HALF, 512), BF),
            vm((SLOTS, HALF, 512), BF),
            vm((SLOTS, TOK, 512), F32),
            vm((SLOTS, TOK, 512), BF),
            vm((2, 3, 512, 256), BF),
            vm((2, 256, 512), BF),
            vm((2, 512, 1024), BF),
            vm((2, 1024, 512), BF),
            vm((4, 256, 512), BF),
            vm((2, 16, 256), F32),
            vm((2, 128, 256), BF),
            vm((13, 512), BF),
            vm((512, 256), BF),
            vm((2, 512, 256), BF),
            vm((256, 512), BF),
            vm((64, 512), F32),
            *[vm(table.shape[1:] if i < 2 else table.shape, table.dtype) for i, table in enumerate(tables)],
            vm((12, 48), jnp.int32),
            vm((12, 48), jnp.int32),
            vm((32, 48), F32),
            vm((TOK, 2048), BF),
            vm((2, 4, 2, 64, 128), F32),
            vm((2, 2, 64, 128), F32),
            vm((1024, 128), F32),
            vm((SLOTS, 2, dests, rows, 128), BF),
            pltpu.SemaphoreType.DMA((20,)),
            pltpu.SemaphoreType.DMA((7,)),
            pltpu.SemaphoreType.DMA((7,)),
            pltpu.SemaphoreType.DMA((SLOTS + 1,)),
            pltpu.SemaphoreType.DMA((SLOTS + 1,)),
            pltpu.SemaphoreType.DMA((SLOTS,)),
            pltpu.SemaphoreType.DMA,
            pltpu.SemaphoreType.REGULAR((4,)),
        ],
        compiler_params=pltpu.CompilerParams(
            collective_id=0, has_side_effects=True, vmem_limit_bytes=60 * 2**20
        ),
    )(*operands)


def assemble(grid, received):
    _, band, _ = sizes(grid)
    tables = final_tables(grid)
    lines = pl.pallas_call(
        functools.partial(final_kernel, grid),
        in_specs=[pl.BlockSpec(memory_space=pltpu.VMEM)] * 3,
        out_shape=jax.ShapeDtypeStruct((NLEV * band, 2, 48 * grid), F32),
        scratch_shapes=[pltpu.VMEM((band, 12 * grid, 128), F32)],
        compiler_params=pltpu.CompilerParams(vmem_limit_bytes=32 * 2**20),
    )(received, *tables)
    return jnp.transpose(lines.reshape(NLEV, band, 2, 48 * grid), (2, 0, 1, 3))


def local(*args):
    grid = lax.axis_size("grid")
    return assemble(grid, pixels_of(grid, *args))


def solution(mesh):
    placed = (
        P("group", "grid", None, None),
        P("group", "grid"),
        P(None, None, "var"),
        P("var", None),
        P(None, "var"),
        P("var", None),
        P(),
        P(None, "var"),
        P(None, None, "var"),
        P("var", None),
        P(),
    )
    return jax.shard_map(
        local, mesh=mesh, in_specs=placed, out_specs=P("var", "group", "grid", None), check_vma=False
    )
```
